32 devices in a mesh: lon: 16 (over z, y, core), band: 2 (over x).
Axes of the slice: x: 2, y: 2, z: 4, core: 2. Of those that a mesh axis runs over, the one named last changes fastest.
Arguments:
- nest_field: float32 [32, 96, 9216], P(None, 'band', 'lon'), may hold values from -6 to 6
- nest_area: float32 [96, 9216], P('band', 'lon'), may hold values from 0.5 to 2
- parent_field: float32 [32, 32, 3072], P(None, 'band', 'lon'), may hold values from -6 to 6
- nest_offset: int32 [1], replicated, may hold values from 576 to 9215
- relax_rate: float32 [32], replicated, may hold values from 0.3 to 0.8
- zonal_coef: float32 [32], replicated, may hold values from 0.05 to 0.24
- merid_coef: float32 [32], replicated, may hold values from 0.05 to 0.24
Outputs:
- parent_out: float32 [32, 32, 3072], P(None, 'band', 'lon')
The draws below stay inside these ranges and needn't reach their ends.
All inputs are finite; a program needn't handle non-finite values.
Results may differ from the reference program's by a relative error of at most 0.000084.
Values sent between devices are 32-bit elements; how exact they have to be, the bound alone decides.
No kernel may reach another device: no remote copies, remote signals or barrier semaphores. Data moves between devices by JAX's collectives and lax.ppermute only.
A program may use at most 64 MiB of HBM per device.

```python
import math
import jax
import jax.numpy as jnp

NXP = 3072
LV = 32
NS = 3
NYP = 32
NYN = 96
NXN = 9216
N_LON = 16


def block_levels(stream_key, shape, split, low, largest):
    def one(axis_at, blocks):
        draws = jax.random.uniform(jax.random.fold_in(jax.random.fold_in(stream_key, 6), axis_at), (blocks,), jnp.float32, low / len(split), largest / len(split))
        return jnp.repeat(jnp.exp(draws), shape[axis_at] // blocks).reshape((-1,) + (1,) * (len(shape) - axis_at - 1))

    level = one(*split[0])
    for cut in split[1:]:
        level = level * one(*cut)
    return level


def centred(key, shape, scale, bound, cuts=(), kind=jnp.bfloat16):
    factor_of = block_levels(key, shape, cuts, -0.22, 0.18) if cuts else 1.0
    result = jax.random.normal(key, shape, jnp.float32) * scale * factor_of
    return jnp.minimum(jnp.maximum(result, -bound), bound).astype(kind)


def setup_inputs(seed: int = 0) -> dict:
    streams_of = jax.random.split(jax.random.key(seed), 8)
    return {
        "nest_field": centred(streams_of[0], (LV, NYN, NXN), 1.0, 6.0, ((1, 2), (2, 16)), jnp.float32),
        "nest_area": jnp.clip(jnp.exp(math.log(2.0) - 1.3862944 * jax.random.uniform(streams_of[1], (NYN, NXN), jnp.float32) ** block_levels(streams_of[1], (NYN, NXN), ((0, 2), (1, 16)), -0.2, 0.2)), 0.5, 2.0),
        "parent_field": centred(streams_of[2], (LV, NYP, NXP), 1.0, 6.0, ((1, 2), (2, 16)), jnp.float32),
        "nest_offset": jax.random.randint(streams_of[3], (1,), 3 * NXP // N_LON, 3 * NXP).astype(jnp.int32),
        "relax_rate": jnp.clip(jax.random.uniform(streams_of[4], (LV,), jnp.float32, 0.3, 0.8), 0.3, 0.8),
        "zonal_coef": jnp.clip(jax.random.uniform(streams_of[5], (LV,), jnp.float32, 0.05, 0.24), 0.05, 0.24),
        "merid_coef": jnp.clip(jax.random.uniform(streams_of[6], (LV,), jnp.float32, 0.05, 0.24), 0.05, 0.24),
    }


def zonal_pass(field, coef):
    left = jnp.roll(field, 1, axis=2)
    right = jnp.roll(field, -1, axis=2)
    return field + coef[:, None, None] * (left - 2.0 * field + right)


def merid_pass(field, coef):
    padded = jnp.pad(field, ((0, 0), (1, 1), (0, 0)))
    return field + coef[:, None, None] * (padded[:, :-2] - 2.0 * field + padded[:, 2:])


def reference(nest_field, nest_area, parent_field, nest_offset, relax_rate, zonal_coef, merid_coef):
    offset_cells = nest_offset[0]
    stacked = jnp.concatenate([nest_field * nest_area[None], nest_area[None]], axis=0)
    planes = stacked.shape[0]
    row_sums = stacked.reshape(planes, NYP, 3, NXN).sum(axis=2)
    rolled = jnp.roll(row_sums, offset_cells, axis=2)
    cell_sums = rolled.reshape(planes, NYP, NXP, 3).sum(axis=3)
    restricted = cell_sums[:LV] / cell_sums[LV][None]
    field = parent_field + relax_rate[:, None, None] * (restricted - parent_field)
    for sweep in range(NS):
        field = zonal_pass(field, zonal_coef)
        field = merid_pass(field, merid_coef)
    return field
```

```python
import functools

import jax
import jax.numpy as jnp
from jax import lax
from jax.experimental import pallas as pl
from jax.experimental.pallas import tpu as pltpu
from jax.sharding import PartitionSpec as P

NS = 3
HALO = 4
LANE = 128
SUB = 8


def lane_blocks(width):
    return -(-width // LANE)


def split_dot(value, selector, parts):
    total = None
    for part in range(parts):
        piece = value.astype(jnp.bfloat16)
        term = jnp.dot(piece, selector, preferred_element_type=jnp.float32)
        total = term if total is None else total + term
        if part + 1 < parts:
            value = value - piece.astype(jnp.float32)
    return total


def restrict_kernel(
    offset_ref, *refs, blocks, nest_width, par_cols, par_rows, frame, level_block, pad_cols
):
    field_refs = refs[:blocks]
    area_refs = refs[blocks : 2 * blocks]
    near_ref, far_ref, before_ref, after_ref, sel_ref, stage_ref = refs[2 * blocks :]
    step = pl.program_id(0)
    offset = offset_ref[0]
    remainder = offset % 3
    place = offset // 3 % par_cols + HALO
    tile = place // SUB
    rows = level_block * par_rows

    def weights(i):
        out = []
        for b in range(blocks):
            a = area_refs[b][pl.ds(i, par_rows, stride=3), :]
            if (b + 1) * LANE > nest_width:
                lanes = lax.broadcasted_iota(jnp.int32, a.shape, 1) + b * LANE
                a = jnp.where(lanes < nest_width, a, 0.0)
            out.append(a)
        return out

    area_at = [weights(i) for i in range(3)]

    @pl.when(step == 0)
    def _():
        g = lax.broadcasted_iota(jnp.int32, (blocks * LANE, pad_cols), 0)
        c = lax.broadcasted_iota(jnp.int32, (blocks * LANE, pad_cols), 1)
        low = 3 * (c - place % SUB) - remainder
        hit = (g >= low) & (g < low + 3) & (g < nest_width)
        sel_ref[...] = jnp.where(hit, 1.0, 0.0).astype(jnp.bfloat16)
        stage_ref[...] = jnp.zeros_like(stage_ref)

        total = jnp.concatenate(
            [area_at[0][b] + area_at[1][b] + area_at[2][b] for b in range(blocks)], axis=1
        )
        compact = split_dot(total, sel_ref[...], 3)
        wide = jnp.concatenate([compact, jnp.zeros_like(compact)], axis=1)
        lanes = lax.broadcasted_iota(jnp.int32, (par_rows, pad_cols), 1)

        def packed(shift):
            moved = pltpu.roll(wide, (tile * SUB + shift + 2 * pad_cols) % (2 * pad_cols), 1)
            part = jnp.where(lanes < frame, moved[:, :pad_cols], 0.0)
            return part

        def put(ref, row, part):
            half = SUB
            pieces = [part[k * half : (k + 1) * half] for k in range(par_rows // half)]
            for k, piece in enumerate(pieces):
                ref[row : row + SUB, k * pad_cols : (k + 1) * pad_cols] = piece

        put(near_ref, frame, packed(0))
        put(far_ref, 0, packed(-par_cols))
        edge = lanes >= par_cols
        put(before_ref, SUB, jnp.where(edge & (tile == 0), packed(par_cols), 0.0))
        last = tile == par_cols // SUB
        put(after_ref, 0, jnp.where((lanes < SUB) & last, packed(-2 * par_cols), 0.0))

    sums = []
    for b in range(blocks):
        acc = None
        for i in range(3):
            f = field_refs[b][:, pl.ds(i, par_rows, stride=3), :]
            if (b + 1) * LANE > nest_width:
                lanes = lax.broadcasted_iota(jnp.int32, f.shape, 2) + b * LANE
                f = jnp.where(lanes < nest_width, f, 0.0)
            term = f * area_at[i][b][None]
            acc = term if acc is None else acc + term
        sums.append(acc.reshape(rows, LANE))
    compact = split_dot(jnp.concatenate(sums, axis=1), sel_ref[...], 2)
    turned = compact.T
    stage_ref[pl.ds(pl.multiple_of(tile * SUB, SUB), frame), :] = turned[:frame]
    near_ref[:frame, pl.ds(pl.multiple_of(step * rows, LANE), rows)] = stage_ref[:frame, :]
    far_ref[SUB:, pl.ds(pl.multiple_of(step * rows, LANE), rows)] = stage_ref[
        par_cols : par_cols + frame, :
    ]
    before_ref[:SUB, pl.ds(pl.multiple_of(step * rows, LANE), rows)] = stage_ref[:SUB, :]
    after_ref[SUB:, pl.ds(pl.multiple_of(step * rows, LANE), rows)] = stage_ref[
        2 * par_cols : 2 * par_cols + SUB, :
    ]


def restrict(nest_field, nest_area, nest_offset, par_cols):
    levels, nest_rows, nest_width = nest_field.shape
    par_rows = nest_rows // 3
    frame = par_cols + 2 * HALO
    pad_cols = lane_blocks(frame) * LANE
    blocks = lane_blocks(nest_width)
    level_block = LANE // par_rows
    span = levels * par_rows
    rows = level_block * par_rows
    field_specs = [
        pl.BlockSpec((level_block, nest_rows, LANE), functools.partial(lambda b, s, o: (s, 0, b), b))
        for b in range(blocks)
    ]
    area_specs = [
        pl.BlockSpec((nest_rows, LANE), functools.partial(lambda b, s, o: (0, b), b))
        for b in range(blocks)
    ]

    def whole(count):
        return pl.BlockSpec((count, span), lambda s, o: (0, 0))

    sizes = (frame + SUB, frame + SUB, 2 * SUB, 2 * SUB)
    return pl.pallas_call(
        functools.partial(
            restrict_kernel,
            blocks=blocks,
            nest_width=nest_width,
            par_cols=par_cols,
            par_rows=par_rows,
            frame=frame,
            level_block=level_block,
            pad_cols=pad_cols,
        ),
        grid_spec=pltpu.PrefetchScalarGridSpec(
            num_scalar_prefetch=1,
            grid=(levels // level_block,),
            in_specs=field_specs + area_specs,
            out_specs=[whole(n) for n in sizes],
            scratch_shapes=[
                pltpu.VMEM((blocks * LANE, pad_cols), jnp.bfloat16),
                pltpu.VMEM((2 * par_cols + SUB, rows), jnp.float32),
            ],
        ),
        out_shape=[jax.ShapeDtypeStruct((n, span), jnp.float32) for n in sizes],
        compiler_params=pltpu.CompilerParams(dimension_semantics=("arbitrary",)),
        name="restrict",
    )(nest_offset, *([nest_field] * blocks), *([nest_area] * blocks))


def edges_kernel(left_ref, right_ref, first_ref, last_ref, *, par_cols):
    span = first_ref.shape[1]
    first_ref[...] = left_ref[...].reshape(span, LANE).T[:SUB]
    low = (par_cols - SUB) % LANE
    last_ref[...] = right_ref[...].reshape(span, LANE).T[low : low + SUB]


def parent_edges(parent):
    levels, par_rows, par_cols = parent.shape
    span = levels * par_rows
    block = (levels, par_rows, LANE)
    last = (par_cols - SUB) // LANE
    return pl.pallas_call(
        functools.partial(edges_kernel, par_cols=par_cols),
        grid=(1,),
        in_specs=[
            pl.BlockSpec(block, lambda i: (0, 0, 0)),
            pl.BlockSpec(block, lambda i: (0, 0, last)),
        ],
        out_specs=[pl.BlockSpec((SUB, span), lambda i: (0, 0))] * 2,
        out_shape=[jax.ShapeDtypeStruct((SUB, span), jnp.float32)] * 2,
        name="edges",
    )(parent, parent)


def zonal_kernel(
    relax_ref, zonal_ref, band_ref, near_ref, far_ref, low_ref, high_ref, parent_ref,
    out_ref, *rest, frame, par_cols, par_rows, levels, pad_cols, starts
):
    edge_refs = rest[: len(starts)]
    num_ref, hal_ref, own_ref, *z_refs = rest[len(starts) :]
    span = levels * par_rows
    tall = pad_cols
    num = near_ref[:frame, :] + far_ref[SUB:, :]
    num = jnp.concatenate([num, jnp.zeros((tall - frame, span), jnp.float32)], axis=0)
    num_ref[...] = num.T
    halo = jnp.concatenate(
        [low_ref[...], high_ref[...], jnp.zeros((LANE - 2 * SUB, span), jnp.float32)], axis=0
    )
    hal_ref[...] = halo.T
    packed = near_ref[frame:, :] + far_ref[:SUB, :]
    area = jnp.concatenate(
        [packed[:, k * pad_cols : (k + 1) * pad_cols] for k in range(par_rows // SUB)], axis=0
    )
    inverse = 1.0 / area
    lanes = lax.broadcasted_iota(jnp.int32, (par_rows, pad_cols), 1)
    own_ref[...] = jnp.zeros_like(own_ref)
    own_ref[:, :, :par_cols] = parent_ref[...]

    def body(level, carry):
        at = pl.multiple_of(level * par_rows, par_rows)
        halo = hal_ref[pl.ds(at, par_rows), :]
        if pad_cols > LANE:
            halo = jnp.concatenate(
                [halo, jnp.zeros((par_rows, pad_cols - LANE), jnp.float32)], axis=1
            )
        own = pltpu.roll(own_ref[level], HALO, 1)
        parent = jnp.where(
            lanes < HALO,
            pltpu.roll(halo, pad_cols - HALO, 1),
            jnp.where(
                lanes < par_cols + HALO, own, pltpu.roll(halo, par_cols + HALO - SUB, 1)
            ),
        )
        restricted = num_ref[pl.ds(at, par_rows), :] * inverse
        field = parent + relax_ref[level] * (restricted - parent)
        coef = zonal_ref[level]
        for _ in range(NS):
            sides = pltpu.roll(field, 1, 1) + pltpu.roll(field, pad_cols - 1, 1)
            field = field + coef * (sides - 2.0 * field)
        field = pltpu.roll(field, pad_cols - HALO, 1)
        out_ref[level] = field[:, :par_cols]
        for k, z_ref in enumerate(z_refs):
            z_ref[pl.ds(at, par_rows), :] = field[:, k * LANE : (k + 1) * LANE]
        return carry

    lax.fori_loop(0, levels, body, 0, unroll=4)
    for edge_ref, (fixed, by_band) in zip(edge_refs, starts):
        for i in range(NS):
            start = fixed + i + (by_band * band_ref[0] if by_band else 0)
            for k, z_ref in enumerate(z_refs):
                edge_ref[i * levels : (i + 1) * levels, k * LANE : (k + 1) * LANE] = z_ref[
                    pl.ds(start, levels, stride=par_rows), :
                ]


def zonal(relax, coef, band, near, far, low, high, parent, starts):
    levels, par_rows, par_cols = parent.shape
    frame = par_cols + 2 * HALO
    pad_cols = lane_blocks(frame) * LANE
    wide = lane_blocks(par_cols)
    span = levels * par_rows
    smem = pl.BlockSpec(memory_space=pltpu.SMEM)
    vmem = pl.BlockSpec(memory_space=pltpu.VMEM)
    edge = jax.ShapeDtypeStruct((NS * levels, wide * LANE), jnp.float32)
    return pl.pallas_call(
        functools.partial(
            zonal_kernel,
            frame=frame,
            par_cols=par_cols,
            par_rows=par_rows,
            levels=levels,
            pad_cols=pad_cols,
            starts=starts,
        ),
        in_specs=[smem] * 3 + [vmem] * 5,
        out_specs=[vmem] * (1 + len(starts)),
        out_shape=[jax.ShapeDtypeStruct(parent.shape, jnp.float32)] + [edge] * len(starts),
        scratch_shapes=[
            pltpu.VMEM((span, pad_cols), jnp.float32),
            pltpu.VMEM((span, LANE), jnp.float32),
            pltpu.VMEM((levels, par_rows, pad_cols), jnp.float32),
        ]
        + [pltpu.VMEM((span, LANE), jnp.float32)] * wide,
        name="zonal",
    )(relax, coef, band, near, far, low, high, parent)


def merid_kernel(
    coef_ref, flag_ref, field_ref, before_ref, after_ref, out_ref, *halo_refs,
    levels, par_rows, par_cols
):
    wide = len(halo_refs) // 2
    keep_before = flag_ref[0].astype(jnp.float32)
    keep_after = flag_ref[1].astype(jnp.float32)
    for k in range(wide):
        for i in range(NS):
            rows = slice(i * levels, (i + 1) * levels)
            cols = slice(k * LANE, (k + 1) * LANE)
            halo_refs[k][pl.ds(SUB - NS + i, levels, stride=SUB), :] = before_ref[rows, cols]
            halo_refs[wide + k][pl.ds(i, levels, stride=SUB), :] = after_ref[rows, cols]

    def body(level, carry):
        at = pl.multiple_of(level * SUB, SUB)
        before = jnp.concatenate([halo_refs[k][pl.ds(at, SUB), :] for k in range(wide)], axis=1)
        after = jnp.concatenate(
            [halo_refs[wide + k][pl.ds(at, SUB), :] for k in range(wide)], axis=1
        )
        mine = jnp.concatenate(
            [
                field_ref[level],
                jnp.zeros((par_rows, wide * LANE - par_cols), jnp.float32),
            ],
            axis=1,
        ) if wide * LANE > par_cols else field_ref[level]
        row = lax.broadcasted_iota(jnp.int32, (par_rows + 2 * SUB, wide * LANE), 0)
        mask = jnp.where(
            row < SUB, keep_before, jnp.where(row < SUB + par_rows, 1.0, keep_after)
        )
        count = par_rows + 2 * SUB
        good = (row >= SUB - NS) & (row < SUB + par_rows + NS)
        field = jnp.where(good, jnp.concatenate([before, mine, after], axis=0), 0.0) * mask
        coef = coef_ref[level]
        for _ in range(NS):
            sides = pltpu.roll(field, 1, 0) + pltpu.roll(field, count - 1, 0)
            field = (field + coef * (sides - 2.0 * field)) * mask
        out_ref[level] = field[SUB : SUB + par_rows, :par_cols]
        return carry

    lax.fori_loop(0, levels, body, 0, unroll=4)


def merid(coef, flags, field, before, after):
    levels, par_rows, par_cols = field.shape
    wide = lane_blocks(par_cols)
    smem = pl.BlockSpec(memory_space=pltpu.SMEM)
    vmem = pl.BlockSpec(memory_space=pltpu.VMEM)
    return pl.pallas_call(
        functools.partial(merid_kernel, levels=levels, par_rows=par_rows, par_cols=par_cols),
        in_specs=[smem] * 2 + [vmem] * 3,
        out_specs=vmem,
        out_shape=jax.ShapeDtypeStruct(field.shape, jnp.float32),
        scratch_shapes=[pltpu.VMEM((levels * SUB, LANE), jnp.float32)] * (2 * wide),
        name="merid",
    )(coef, flags, field, before, after)


def turn(value, steps):
    count = lax.axis_size("lon")
    return lax.ppermute(value, "lon", [(i, (i + steps) % count) for i in range(count)])


def bins_of(frame):
    quantum = 5 * SUB
    return quantum, -(-frame // quantum)


def on_device(nest_field, nest_area, parent_field, nest_offset, relax_rate, zonal_coef, merid_coef):
    par_cols = parent_field.shape[2]
    par_rows = parent_field.shape[1]
    frame = par_cols + 2 * HALO
    cycle = lax.axis_size("lon")
    bands = lax.axis_size("band")
    band = lax.axis_index("band").astype(jnp.int32)

    first, last = parent_edges(parent_field)
    low = turn(last, 1)
    high = turn(first, -1)
    near, far, before, after = restrict(nest_field, nest_area, nest_offset, par_cols)

    quantum, bins = bins_of(frame)
    places = nest_offset[0] // 3
    steps = places // par_cols % cycle
    slot = (places % par_cols + HALO) // quantum

    def branch(step, number):
        start = number * quantum
        count = min(start + quantum, frame)

        def send(near, far, before, after):
            got_near = turn(near[start:], step)
            got_far = turn(far[: SUB + count], step + 1)
            got_near = jnp.pad(got_near, ((start, 0), (0, 0)))
            got_far = jnp.pad(got_far, ((0, frame - count), (0, 0)))
            if number == 0:
                got_near = got_near.at[par_cols + 2 * HALO - SUB :].add(turn(before, step - 1))
            if number == bins - 1:
                got_far = got_far.at[: 2 * SUB].add(turn(after, step + 2))
            return got_near, got_far

        return send

    branches = [branch(step, number) for step in range(cycle) for number in range(bins)]
    near, far = lax.switch(steps * bins + slot, branches, near, far, before, after)

    if bands == 2:
        starts = ((par_rows - NS, -(par_rows - NS)),)
    else:
        starts = ((par_rows - NS, 0), (0, 0))
    field, *edges = zonal(
        relax_rate, zonal_coef, band[None], near, far, low, high, parent_field, starts
    )
    if bands == 2:
        other = lax.ppermute(edges[0], "band", [(0, 1), (1, 0)])
        north, south = other, other
    else:
        north = lax.ppermute(edges[0], "band", [(i, i + 1) for i in range(bands - 1)])
        south = lax.ppermute(edges[1], "band", [(i + 1, i) for i in range(bands - 1)])
    flags = jnp.stack([band > 0, band < bands - 1]).astype(jnp.int32)
    return merid(merid_coef, flags, field, north, south)


def solution(mesh):
    placed = (P(None, "band", "lon"), P("band", "lon"), P(None, "band", "lon"), P(), P(), P(), P())
    return jax.shard_map(
        on_device, mesh=mesh, in_specs=placed, out_specs=P(None, "band", "lon"), check_vma=False
    )
```

```python
import functools

import jax
import jax.numpy as jnp
from jax import lax
from jax.experimental import pallas as pl
from jax.experimental.pallas import tpu as pltpu
from jax.sharding import PartitionSpec as P

NS = 3
HALO = 4
LANE = 128
VMEM_LIMIT = 16 << 20
QUANTUM = 40
SUB = 8


def lane_blocks(width):
    return -(-width // LANE)


def split_dot(value, selector, parts):
    total = None
    for part in range(parts):
        piece = value.astype(jnp.bfloat16)
        term = jnp.dot(piece, selector, preferred_element_type=jnp.float32)
        total = term if total is None else total + term
        if part + 1 < parts:
            value = value - piece.astype(jnp.float32)
    return total


def restrict_kernel(
    offset_ref, *refs, blocks, nest_width, par_cols, par_rows, frame, chunks, pad_cols, levels
):
    field_refs = refs[:blocks]
    area_refs = refs[blocks : 2 * blocks]
    parent_ref = refs[2 * blocks]
    near_ref, far_ref, before_ref, after_ref, first_ref, last_ref = refs[
        2 * blocks + 1 : 2 * blocks + 7
    ]
    sel_ref, stage_ref, own_ref, own_sem = refs[2 * blocks + 7 :]
    step = pl.program_id(0)
    offset = offset_ref[0]
    remainder = offset % 3
    place = offset // 3 % par_cols + HALO
    tile = place // SUB
    level_block = LANE // par_rows
    fetch = pltpu.make_async_copy(parent_ref, own_ref, own_sem)

    def weights(i):
        out = []
        for b in range(blocks):
            a = area_refs[b][pl.ds(i, par_rows, stride=3), :]
            if (b + 1) * LANE > nest_width:
                lanes = lax.broadcasted_iota(jnp.int32, a.shape, 1) + b * LANE
                a = jnp.where(lanes < nest_width, a, 0.0)
            out.append(a)
        return out

    area_at = [weights(i) for i in range(3)]

    @pl.when(step == 0)
    def _():
        fetch.start()
        g = lax.broadcasted_iota(jnp.int32, (blocks * LANE, pad_cols), 0)
        c = lax.broadcasted_iota(jnp.int32, (blocks * LANE, pad_cols), 1)
        low = 3 * (c - place % SUB) - remainder
        hit = (g >= low) & (g < low + 3) & (g < nest_width)
        sel_ref[...] = jnp.where(hit, 1.0, 0.0).astype(jnp.bfloat16)
        stage_ref[...] = jnp.zeros_like(stage_ref)

        total = jnp.concatenate(
            [area_at[0][b] + area_at[1][b] + area_at[2][b] for b in range(blocks)], axis=1
        )
        compact = split_dot(total, sel_ref[...], 3)
        wide = jnp.concatenate([compact, jnp.zeros_like(compact)], axis=1)
        lanes = lax.broadcasted_iota(jnp.int32, (par_rows, pad_cols), 1)

        def packed(shift):
            moved = pltpu.roll(wide, (tile * SUB + shift + 2 * pad_cols) % (2 * pad_cols), 1)
            return jnp.where(lanes < frame, moved[:, :pad_cols], 0.0)

        def put(ref, row, part):
            ref[row : row + SUB, :] = jnp.zeros((SUB, ref.shape[1]), jnp.float32)
            for k in range(par_rows // SUB):
                ref[row : row + SUB, k * pad_cols : (k + 1) * pad_cols] = part[
                    k * SUB : (k + 1) * SUB
                ]

        put(near_ref, frame, packed(0))
        put(far_ref, 0, packed(-par_cols))
        edge = lanes >= par_cols
        put(before_ref, SUB, jnp.where(edge & (tile == 0), packed(par_cols), 0.0))
        last = tile == par_cols // SUB
        put(after_ref, 0, jnp.where((lanes < SUB) & last, packed(-2 * par_cols), 0.0))

    for chunk in range(chunks):
        sums = []
        for b in range(blocks):
            acc = None
            for i in range(3):
                f = field_refs[b][
                    chunk * level_block : (chunk + 1) * level_block, pl.ds(i, par_rows, stride=3), :
                ]
                if (b + 1) * LANE > nest_width:
                    lanes = lax.broadcasted_iota(jnp.int32, f.shape, 2) + b * LANE
                    f = jnp.where(lanes < nest_width, f, 0.0)
                term = f * area_at[i][b][None]
                acc = term if acc is None else acc + term
            sums.append(acc.reshape(LANE, LANE))
        compact = split_dot(jnp.concatenate(sums, axis=1), sel_ref[...], 2)
        turned = compact.T
        stage_ref[chunk, pl.ds(pl.multiple_of(tile * SUB, SUB), frame), :] = turned[:frame]
        cols = pl.ds(pl.multiple_of((step * chunks + chunk) * LANE, LANE), LANE)
        near_ref[:frame, cols] = stage_ref[chunk, :frame, :]
        far_ref[SUB:, cols] = stage_ref[chunk, par_cols : par_cols + frame, :]
        before_ref[:SUB, cols] = stage_ref[chunk, :SUB, :]
        after_ref[SUB:, cols] = stage_ref[chunk, 2 * par_cols : 2 * par_cols + SUB, :]

    @pl.when(step == pl.num_programs(0) - 1)
    def _():
        fetch.wait()
        span = levels * par_rows
        low = (par_cols - SUB) // LANE * LANE
        wide = min(LANE, par_cols)
        left = own_ref[:, :, :wide].reshape(span, wide)
        right = own_ref[:, :, low:].reshape(span, par_cols - low)
        first_ref[...] = left.T[:SUB]
        last_ref[...] = right.T[par_cols - low - SUB :]


def restrict(nest_field, nest_area, nest_offset, parent):
    levels, nest_rows, nest_width = nest_field.shape
    par_cols = parent.shape[2]
    par_rows = nest_rows // 3
    frame = par_cols + 2 * HALO
    pad_cols = lane_blocks(frame) * LANE
    blocks = lane_blocks(nest_width)
    level_block = LANE // par_rows
    span = levels * par_rows
    chunks = 2 if levels % (2 * level_block) == 0 else 1
    take = chunks * level_block
    field_specs = [
        pl.BlockSpec((take, nest_rows, LANE), functools.partial(lambda b, s, o: (s, 0, b), b))
        for b in range(blocks)
    ]
    area_specs = [
        pl.BlockSpec((nest_rows, LANE), functools.partial(lambda b, s, o: (0, b), b))
        for b in range(blocks)
    ]

    def whole(count):
        return pl.BlockSpec((count, span), lambda s, o: (0, 0))

    sizes = (frame + SUB, frame + SUB, 2 * SUB, 2 * SUB, SUB, SUB)
    return pl.pallas_call(
        functools.partial(
            restrict_kernel,
            blocks=blocks,
            nest_width=nest_width,
            par_cols=par_cols,
            par_rows=par_rows,
            frame=frame,
            chunks=chunks,
            pad_cols=pad_cols,
            levels=levels,
        ),
        grid_spec=pltpu.PrefetchScalarGridSpec(
            num_scalar_prefetch=1,
            grid=(levels // take,),
            in_specs=field_specs + area_specs + [pl.BlockSpec(memory_space=pl.ANY)],
            out_specs=[whole(n) for n in sizes],
            scratch_shapes=[
                pltpu.VMEM((blocks * LANE, pad_cols), jnp.bfloat16),
                pltpu.VMEM((chunks, 2 * par_cols + SUB, LANE), jnp.float32),
                pltpu.VMEM(parent.shape, jnp.float32),
                pltpu.SemaphoreType.DMA,
            ],
        ),
        out_shape=[jax.ShapeDtypeStruct((n, span), jnp.float32) for n in sizes],
        compiler_params=pltpu.CompilerParams(dimension_semantics=("arbitrary",)),
        name="restrict",
    )(nest_offset, *([nest_field] * blocks), *([nest_area] * blocks), parent)


def bin_start(offset, par_cols):
    place = lax.rem(lax.div(offset, 3), par_cols) + HALO
    return lax.div(place, QUANTUM) * QUANTUM


def zonal_kernel(
    offset_ref, band_ref, relax_ref, zonal_ref, got_ref, low_ref, high_ref, parent_ref,
    out_ref, *rest, frame, par_cols, par_rows, pad_cols, starts
):
    edge_refs = rest[: len(starts)]
    z_refs = rest[len(starts) :]
    levels = parent_ref.shape[0]
    start = bin_start(offset_ref[0], par_cols)
    level_block = LANE // par_rows
    count = got_ref.shape[0]
    packed = got_ref[:SUB, :] + got_ref[count - SUB :, :]
    area = jnp.concatenate(
        [packed[:, k * pad_cols : (k + 1) * pad_cols] for k in range(par_rows // SUB)], axis=0
    )
    inverse = 1.0 / area
    lanes = lax.broadcasted_iota(jnp.int32, (par_rows, pad_cols), 1)
    rows = lax.broadcasted_iota(jnp.int32, (frame, LANE), 0)

    def body(chunk, carry):
        cols = pl.ds(pl.multiple_of(chunk * LANE, LANE), LANE)
        num = jnp.where(rows < start + QUANTUM, got_ref[SUB : SUB + frame, cols], 0.0) + jnp.where(
            rows >= start, got_ref[SUB + QUANTUM : SUB + QUANTUM + frame, cols], 0.0
        )
        num = jnp.concatenate([num, jnp.zeros((pad_cols - frame, LANE), jnp.float32)], axis=0).T
        halo = jnp.concatenate(
            [low_ref[:, cols], high_ref[:, cols], jnp.zeros((LANE - 2 * SUB, LANE), jnp.float32)],
            axis=0,
        ).T
        for k in range(level_block):
            level = chunk * level_block + k
            at = slice(k * par_rows, (k + 1) * par_rows)
            edge = halo[at]
            own = parent_ref[level]
            if pad_cols > par_cols:
                own = jnp.concatenate(
                    [own, jnp.zeros((par_rows, pad_cols - par_cols), jnp.float32)], axis=1
                )
            if pad_cols > LANE:
                edge = jnp.concatenate(
                    [edge, jnp.zeros((par_rows, pad_cols - LANE), jnp.float32)], axis=1
                )
            parent = jnp.where(
                lanes < HALO,
                pltpu.roll(edge, pad_cols - HALO, 1),
                jnp.where(
                    lanes < par_cols + HALO,
                    pltpu.roll(own, HALO, 1),
                    pltpu.roll(edge, par_cols + HALO - SUB, 1),
                ),
            )
            field = parent + relax_ref[level] * (num[at] * inverse - parent)
            coef = zonal_ref[level]
            for _ in range(NS):
                sides = pltpu.roll(field, 1, 1) + pltpu.roll(field, pad_cols - 1, 1)
                field = field + coef * (sides - 2.0 * field)
            field = pltpu.roll(field, pad_cols - HALO, 1)
            out_ref[level] = field[:, :par_cols]
            for w, z_ref in enumerate(z_refs):
                z_ref[pl.ds(pl.multiple_of(level * par_rows, par_rows), par_rows), :] = field[
                    :, w * LANE : (w + 1) * LANE
                ]
        return carry

    lax.fori_loop(0, levels // level_block, body, 0)
    for edge_ref, (fixed, by_band) in zip(edge_refs, starts):
        for i in range(NS):
            base = fixed + i + (by_band * band_ref[0] if by_band else 0)
            for w, z_ref in enumerate(z_refs):
                edge_ref[i, :, w * LANE : (w + 1) * LANE] = z_ref[
                    pl.ds(base, levels, stride=par_rows), :
                ]


def zonal(offset, band, relax, coef, got, low, high, parent, starts):
    levels, par_rows, par_cols = parent.shape
    frame = par_cols + 2 * HALO
    pad_cols = lane_blocks(frame) * LANE
    wide = lane_blocks(par_cols)
    smem = pl.BlockSpec(memory_space=pltpu.SMEM)
    vmem = pl.BlockSpec(memory_space=pltpu.VMEM)
    edge = jax.ShapeDtypeStruct((NS, levels, wide * LANE), jnp.float32)
    return pl.pallas_call(
        functools.partial(
            zonal_kernel,
            frame=frame,
            par_cols=par_cols,
            par_rows=par_rows,
            pad_cols=pad_cols,
            starts=starts,
        ),
        in_specs=[smem] * 4 + [vmem] * 4,
        out_specs=[vmem] * (1 + len(starts)),
        out_shape=[jax.ShapeDtypeStruct(parent.shape, jnp.float32)] + [edge] * len(starts),
        scratch_shapes=[pltpu.VMEM((levels * par_rows, LANE), jnp.float32)] * wide,
        compiler_params=pltpu.CompilerParams(vmem_limit_bytes=VMEM_LIMIT),
        name="zonal",
    )(offset, band, relax, coef, got, low, high, parent)


def merid_kernel(
    coef_ref, band_ref, field_ref, before_ref, after_ref, out_ref, *halo_refs,
    par_rows, par_cols, bands
):
    wide = len(halo_refs) // 2
    levels = field_ref.shape[0]
    band = band_ref[0]
    keep_before = jnp.where(band > 0, 1.0, 0.0)
    keep_after = jnp.where(band < bands - 1, 1.0, 0.0)
    for k in range(wide):
        for i in range(NS):
            cols = slice(k * LANE, (k + 1) * LANE)
            halo_refs[k][pl.ds(SUB - NS + i, levels, stride=SUB), :] = before_ref[i, :, cols]
            halo_refs[wide + k][pl.ds(i, levels, stride=SUB), :] = after_ref[i, :, cols]
    row = lax.broadcasted_iota(jnp.int32, (SUB, wide * LANE), 0)

    def body(level, carry):
        at = pl.ds(pl.multiple_of(level * SUB, SUB), SUB)
        before = jnp.concatenate([r[at, :] for r in halo_refs[:wide]], axis=1)
        after = jnp.concatenate([r[at, :] for r in halo_refs[wide:]], axis=1)
        mine = field_ref[level]
        if wide * LANE > par_cols:
            mine = jnp.concatenate(
                [mine, jnp.zeros((par_rows, wide * LANE - par_cols), jnp.float32)], axis=1
            )
        tiles = [jnp.where((row >= SUB - NS) & (band > 0), before, 0.0)]
        tiles += [mine[j * SUB : (j + 1) * SUB] for j in range(par_rows // SUB)]
        tiles += [jnp.where((row < NS) & (band < bands - 1), after, 0.0)]
        coef = coef_ref[level]
        for sweep in range(NS):
            down = [pltpu.roll(t, 1, 0) for t in tiles]
            up = [pltpu.roll(t, SUB - 1, 0) for t in tiles]
            fresh = []
            for j, t in enumerate(tiles):
                prev = jnp.where(row == 0, down[j - 1], down[j]) if j else down[j]
                succ = jnp.where(row == SUB - 1, up[j + 1], up[j]) if j + 1 < len(tiles) else up[j]
                fresh.append(t + coef * (prev + succ - 2.0 * t))
            tiles = fresh
            if sweep + 1 < NS:
                tiles[0] = tiles[0] * keep_before
                tiles[-1] = tiles[-1] * keep_after
        out_ref[level] = jnp.concatenate(tiles[1:-1], axis=0)[:, :par_cols]
        return carry

    lax.fori_loop(0, levels, body, 0, unroll=8)


def merid(coef, band, field, before, after, bands):
    levels, par_rows, par_cols = field.shape
    wide = lane_blocks(par_cols)
    smem = pl.BlockSpec(memory_space=pltpu.SMEM)
    vmem = pl.BlockSpec(memory_space=pltpu.VMEM)
    return pl.pallas_call(
        functools.partial(merid_kernel, par_rows=par_rows, par_cols=par_cols, bands=bands),
        in_specs=[smem] * 2 + [vmem] * 3,
        out_specs=vmem,
        out_shape=jax.ShapeDtypeStruct(field.shape, jnp.float32),
        scratch_shapes=[pltpu.VMEM((levels * SUB, LANE), jnp.float32)] * (2 * wide),
        compiler_params=pltpu.CompilerParams(vmem_limit_bytes=VMEM_LIMIT),
        name="merid",
    )(coef, band, field, before, after)


def turn(value, steps):
    count = lax.axis_size("lon")
    return lax.ppermute(value, "lon", [(i, (i + steps) % count) for i in range(count)])


def on_device(nest_field, nest_area, parent_field, nest_offset, relax_rate, zonal_coef, merid_coef):
    levels, par_rows, par_cols = parent_field.shape
    frame = par_cols + 2 * HALO
    cycle = lax.axis_size("lon")
    bands = lax.axis_size("band")
    span = levels * par_rows

    places = lax.div(nest_offset[0], 3)
    steps = lax.rem(lax.div(places, par_cols), cycle)
    slot = lax.div(lax.rem(places, par_cols) + HALO, QUANTUM)
    band = lax.axis_index("band").astype(jnp.int32)[None]
    bins = -(-frame // QUANTUM)

    near, far, before, after, first, last = restrict(
        nest_field, nest_area, nest_offset, parent_field
    )
    low = turn(last, 1)
    high = turn(first, -1)

    def branch(step, number):
        start = number * QUANTUM
        count = min(start + QUANTUM, frame)

        def send(near, far, before, after):
            got_near = turn(near[start:], step)
            got_far = turn(far[: SUB + count], step + 1)
            if number == 0:
                cut = par_cols + 2 * HALO - SUB
                got_near = jnp.concatenate(
                    [got_near[:cut], got_near[cut:] + turn(before, step - 1)], axis=0
                )
            if number == bins - 1:
                cut = 2 * SUB
                got_far = jnp.concatenate(
                    [got_far[:cut] + turn(after, step + 2), got_far[cut:]], axis=0
                )
            gap = start + QUANTUM - count
            pieces = [got_far] + ([jnp.zeros((gap, span), jnp.float32)] if gap else []) + [got_near]
            return jnp.concatenate(pieces, axis=0)

        return send

    branches = [branch(step, number) for step in range(cycle) for number in range(bins)]
    got = lax.switch(steps * bins + slot, branches, near, far, before, after)

    if bands == 2:
        starts = ((par_rows - NS, -(par_rows - NS)),)
    else:
        starts = ((par_rows - NS, 0), (0, 0))
    field, *edges = zonal(
        nest_offset, band, relax_rate, zonal_coef, got, low, high, parent_field, starts
    )
    if bands == 2:
        other = lax.ppermute(edges[0], "band", [(0, 1), (1, 0)])
        north, south = other, other
    else:
        north = lax.ppermute(edges[0], "band", [(i, i + 1) for i in range(bands - 1)])
        south = lax.ppermute(edges[1], "band", [(i + 1, i) for i in range(bands - 1)])
    return merid(merid_coef, band, field, north, south, bands)


def solution(mesh):
    placed = (P(None, "band", "lon"), P("band", "lon"), P(None, "band", "lon"), P(), P(), P(), P())
    return jax.shard_map(
        on_device, mesh=mesh, in_specs=placed, out_specs=P(None, "band", "lon"), check_vma=False
    )
```

```python
import functools
import math

import jax
import jax.numpy as jnp
from jax import lax
from jax.experimental import pallas as pl
from jax.experimental.pallas import tpu as pltpu
from jax.sharding import PartitionSpec as P

NS = 3
BINOMIAL = [math.comb(NS, p) for p in range(NS + 1)]
HALO = 4
LANE = 128
VMEM_LIMIT = 16 << 20
QUANTUM = 40
SUB = 8


def lane_blocks(width):
    return -(-width // LANE)


def split_dot(value, selector, parts):
    total = None
    for part in range(parts):
        piece = value.astype(jnp.bfloat16)
        term = jnp.dot(piece, selector, preferred_element_type=jnp.float32)
        total = term if total is None else total + term
        if part + 1 < parts:
            value = value - piece.astype(jnp.float32)
    return total


def zonal_matrix(frame, par_cols, pad_cols, power):
    lane = lax.broadcasted_iota(jnp.int32, (pad_cols, pad_cols), 0)
    target = lax.broadcasted_iota(jnp.int32, (pad_cols, pad_cols), 1)
    low = frame + SUB - HALO
    column = jnp.where(
        lane < frame,
        lane,
        jnp.where(
            (lane >= low) & (lane < frame + SUB),
            lane - low,
            jnp.where(
                (lane >= frame + SUB) & (lane < frame + SUB + HALO),
                lane - SUB - HALO,
                -pad_cols,
            ),
        ),
    )
    apart = jnp.abs(column - HALO - target)
    weights = [1]
    for _ in range(power):
        weights = [
            x - 2 * y + z
            for x, y, z in zip([0, 0] + weights, [0] + weights + [0], weights + [0, 0])
        ]
    out = jnp.zeros((pad_cols, pad_cols), jnp.float32)
    for distance in range(power + 1):
        out = jnp.where(apart == distance, float(weights[power + distance]), out)
    return jnp.where(target < par_cols, out, 0.0).astype(jnp.bfloat16)


def restrict_kernel(
    offset_ref, area_hbm, nest_ref, parent_ref,
    near_ref, far_ref, spill_ref, mat_hbm,
    mat_ref, sel_ref, stage_ref, area_ref, own_ref, raw_ref, prod_ref, side_sem, raw_sem,
    *, blocks, nest_width, par_cols, par_rows, frame, chunks, pad_cols, levels
):
    level_block = LANE // par_rows
    nest_rows = 3 * par_rows

    def fetch(chunk):
        part = pl.ds(chunk * level_block, level_block)
        return pltpu.make_async_copy(nest_ref.at[part], raw_ref.at[part], raw_sem.at[chunk])

    area_copy = pltpu.make_async_copy(area_hbm, area_ref, side_sem.at[0])
    own_copy = pltpu.make_async_copy(parent_ref, own_ref, side_sem.at[1])
    area_copy.start()
    for chunk in range(chunks):
        fetch(chunk).start()
    own_copy.start()

    offset = offset_ref[0]
    remainder = offset % 3
    place = offset // 3 % par_cols + HALO
    tile = place // SUB
    g = lax.broadcasted_iota(jnp.int32, (blocks * LANE, pad_cols), 0)
    c = lax.broadcasted_iota(jnp.int32, (blocks * LANE, pad_cols), 1)
    low = 3 * (c - place % SUB) - remainder
    hit = (g >= low) & (g < low + 3) & (g < nest_width)
    sel_ref[...] = jnp.where(hit, 1.0, 0.0).astype(jnp.bfloat16)
    for power in range(NS + 1):
        mat_ref[:, power * pad_cols : (power + 1) * pad_cols] = zonal_matrix(
            frame, par_cols, pad_cols, power
        )
    mat_copy = pltpu.make_async_copy(mat_ref, mat_hbm, side_sem.at[2])
    mat_copy.start()
    stage_ref[...] = jnp.zeros_like(stage_ref)

    def columns(value, b):
        width = min(LANE, nest_width - b * LANE)
        piece = value[..., b * LANE : b * LANE + width]
        if width == LANE:
            return piece
        return jnp.concatenate(
            [piece, jnp.zeros(piece.shape[:-1] + (LANE - width,), jnp.float32)], axis=-1
        )

    def row_sums(b, count):
        total = None
        for i in range(3):
            term = prod_ref[b, pl.ds(i, count, stride=3), :]
            total = term if total is None else total + term
        return total

    area_copy.wait()
    for b in range(blocks):
        prod_ref[b, :nest_rows, :] = columns(area_ref[...], b)
    total = jnp.concatenate([row_sums(b, par_rows) for b in range(blocks)], axis=1)
    compact = split_dot(total, sel_ref[...], 3)
    wide = jnp.concatenate([compact, jnp.zeros_like(compact)], axis=1)
    lanes = lax.broadcasted_iota(jnp.int32, (par_rows, pad_cols), 1)

    def packed(shift):
        moved = pltpu.roll(wide, (tile * SUB + shift + 2 * pad_cols) % (2 * pad_cols), 1)
        return jnp.where(lanes < frame, moved[:, :pad_cols], 0.0)

    def put(ref, row, part):
        ref[row : row + SUB, :] = jnp.zeros((SUB, ref.shape[1]), jnp.float32)
        for k in range(par_rows // SUB):
            ref[row : row + SUB, k * pad_cols : (k + 1) * pad_cols] = part[
                k * SUB : (k + 1) * SUB
            ]

    put(near_ref, frame, packed(0))
    put(far_ref, 0, packed(-par_cols))
    edge = lanes >= par_cols
    put(spill_ref, SUB, jnp.where(edge & (tile == 0), packed(par_cols), 0.0))
    last = tile == par_cols // SUB
    put(spill_ref, 2 * SUB, jnp.where((lanes < SUB) & last, packed(-2 * par_cols), 0.0))

    for chunk in range(chunks):
        fetch(chunk).wait()
        for b in range(blocks):
            area = columns(area_ref[...], b)
            for k in range(level_block):
                prod_ref[b, k * nest_rows : (k + 1) * nest_rows, :] = area * columns(
                    raw_ref[chunk * level_block + k], b
                )
        sums = jnp.concatenate([row_sums(b, LANE) for b in range(blocks)], axis=1)
        turned = split_dot(sums, sel_ref[...], 2).T
        stage_ref[pl.ds(pl.multiple_of(tile * SUB, SUB), frame), :] = turned[:frame]
        cols = slice(chunk * LANE, (chunk + 1) * LANE)
        near_ref[:frame, cols] = stage_ref[:frame, :]
        far_ref[SUB:, cols] = stage_ref[par_cols : par_cols + frame, :]
        spill_ref[:SUB, cols] = stage_ref[:SUB, :]
        spill_ref[3 * SUB : 4 * SUB, cols] = stage_ref[2 * par_cols : 2 * par_cols + SUB, :]

    own_copy.wait()
    span = levels * par_rows
    low = (par_cols - SUB) // LANE * LANE
    wide = min(LANE, par_cols)
    left = own_ref[:, :, :wide].reshape(span, wide)
    right = own_ref[:, :, low:].reshape(span, par_cols - low)
    spill_ref[4 * SUB : 5 * SUB, :] = left.T[:SUB]
    spill_ref[5 * SUB :, :] = right.T[par_cols - low - SUB :]
    mat_copy.wait()


def padded_width(frame):
    return lane_blocks(frame + 2 * SUB) * LANE


def restrict(nest_field, nest_area, nest_offset, parent):
    levels, nest_rows, nest_width = nest_field.shape
    par_cols = parent.shape[2]
    par_rows = nest_rows // 3
    frame = par_cols + 2 * HALO
    pad_cols = padded_width(frame)
    blocks = lane_blocks(nest_width)
    level_block = LANE // par_rows
    span = levels * par_rows
    chunks = levels // level_block
    smem = pl.BlockSpec(memory_space=pltpu.SMEM)
    vmem = pl.BlockSpec(memory_space=pltpu.VMEM)
    away = pl.BlockSpec(memory_space=pltpu.HBM)
    sizes = (frame + SUB, frame + SUB, 6 * SUB)
    return pl.pallas_call(
        functools.partial(
            restrict_kernel,
            blocks=blocks,
            nest_width=nest_width,
            par_cols=par_cols,
            par_rows=par_rows,
            frame=frame,
            chunks=chunks,
            pad_cols=pad_cols,
            levels=levels,
        ),
        in_specs=[smem, away, away, away],
        out_specs=[vmem] * len(sizes) + [away],
        out_shape=[jax.ShapeDtypeStruct((n, span), jnp.float32) for n in sizes]
        + [jax.ShapeDtypeStruct((pad_cols, (NS + 1) * pad_cols), jnp.bfloat16)],
        scratch_shapes=[
            pltpu.VMEM((pad_cols, (NS + 1) * pad_cols), jnp.bfloat16),
            pltpu.VMEM((blocks * LANE, pad_cols), jnp.bfloat16),
            pltpu.VMEM((2 * par_cols + SUB, LANE), jnp.float32),
            pltpu.VMEM(nest_area.shape, jnp.float32),
            pltpu.VMEM(parent.shape, jnp.float32),
            pltpu.VMEM(nest_field.shape, jnp.float32),
            pltpu.VMEM((blocks, level_block * nest_rows, LANE), jnp.float32),
            pltpu.SemaphoreType.DMA((3,)),
            pltpu.SemaphoreType.DMA((chunks,)),
        ],
        name="restrict",
    )(nest_offset, nest_area, nest_field, parent)


def bin_start(offset, par_cols):
    place = lax.rem(lax.div(offset, 3), par_cols) + HALO
    return lax.div(place, QUANTUM) * QUANTUM


def zonal_kernel(
    offset_ref, band_ref, relax_ref, zonal_ref, merid_ref, got_ref, low_ref, high_ref, parent_ref,
    mat_ref, out_ref, coef_ref, *rest, frame, par_cols, par_rows, pad_cols, starts
):
    edge_refs = rest[: len(starts)]
    num_ref, pow_ref, table_ref, table_sem, *z_refs = rest[len(starts) :]
    levels = parent_ref.shape[0]
    fetches = [
        pltpu.make_async_copy(source, table_ref.at[k], table_sem.at[k])
        for k, source in enumerate((relax_ref, zonal_ref, merid_ref))
    ]
    for fetch in fetches:
        fetch.start()
    start = bin_start(offset_ref[0], par_cols)
    level_block = LANE // par_rows
    chunks = levels // level_block
    count = got_ref.shape[0]
    packed = got_ref[:SUB, :] + got_ref[count - SUB :, :]
    area = jnp.concatenate(
        [packed[:, k * pad_cols : (k + 1) * pad_cols] for k in range(par_rows // SUB)], axis=0
    )
    inverse = 1.0 / area
    inside = lax.broadcasted_iota(jnp.int32, (par_rows, pad_cols), 1) < frame
    rows = lax.broadcasted_iota(jnp.int32, (frame, LANE), 0)
    for chunk in range(chunks):
        cols = slice(chunk * LANE, (chunk + 1) * LANE)
        num = jnp.where(rows < start + QUANTUM, got_ref[SUB : SUB + frame, cols], 0.0) + jnp.where(
            rows >= start, got_ref[SUB + QUANTUM : SUB + QUANTUM + frame, cols], 0.0
        )
        rest_rows = pad_cols - frame - 2 * SUB
        num_ref[cols, :] = jnp.concatenate(
            [num, low_ref[:, cols], high_ref[:, cols], jnp.zeros((rest_rows, LANE), jnp.float32)],
            axis=0,
        ).T
    for fetch in fetches:
        fetch.wait()
    for chunk in range(chunks):
        fields = []
        for k in range(level_block):
            level = chunk * level_block + k
            relax = table_ref[0, level]
            own = parent_ref[level]
            own = jnp.concatenate(
                [own, jnp.zeros((par_rows, pad_cols - par_cols), jnp.float32)], axis=1
            )
            own = pltpu.roll(own, HALO, 1)
            scale = jnp.where(inside, relax * inverse, 1.0 - relax)
            at = slice(level * par_rows, (level + 1) * par_rows)
            fields.append(num_ref[at, :] * scale + (1.0 - relax) * own)
        field = jnp.concatenate(fields, axis=0)
        high = field.astype(jnp.bfloat16)
        low = (field - high.astype(jnp.float32)).astype(jnp.bfloat16)
        pow_ref[chunk * LANE : (chunk + 1) * LANE, :] = jnp.dot(
            high, mat_ref[...], preferred_element_type=jnp.float32
        ) + jnp.dot(low, mat_ref[...], preferred_element_type=jnp.float32)
    for level in range(levels):
        coef = table_ref[1, level]
        at = slice(level * par_rows, (level + 1) * par_rows)
        term = [pow_ref[at, p * pad_cols : p * pad_cols + par_cols] for p in range(NS + 1)]
        field = term[0]
        for p in range(1, NS + 1):
            field = field + (coef**p * float(BINOMIAL[p])) * term[p]
        out_ref[level] = field
        coef_ref[level : level + 1, :] = jnp.full((1, LANE), table_ref[2, level], jnp.float32)
        for w, z_ref in enumerate(z_refs):
            width = min(LANE, par_cols - w * LANE)
            z_ref[at, :width] = field[:, w * LANE : w * LANE + width]
    for edge_ref, (fixed, by_band) in zip(edge_refs, starts):
        for i in range(NS):
            base = fixed + i + (by_band * band_ref[0] if by_band else 0)
            for w, z_ref in enumerate(z_refs):
                edge_ref[i, :, w * LANE : (w + 1) * LANE] = z_ref[
                    pl.ds(base, levels, stride=par_rows), :
                ]


def zonal(offset, band, relax, coef, merid_coef, got, low, high, parent, matrix, starts):
    levels, par_rows, par_cols = parent.shape
    frame = par_cols + 2 * HALO
    pad_cols = padded_width(frame)
    wide = lane_blocks(par_cols)
    span = levels * par_rows
    smem = pl.BlockSpec(memory_space=pltpu.SMEM)
    vmem = pl.BlockSpec(memory_space=pltpu.VMEM)
    anywhere = pl.BlockSpec(memory_space=pl.ANY)
    edge = jax.ShapeDtypeStruct((NS, levels, wide * LANE), jnp.float32)
    return pl.pallas_call(
        functools.partial(
            zonal_kernel,
            frame=frame,
            par_cols=par_cols,
            par_rows=par_rows,
            pad_cols=pad_cols,
            starts=starts,
        ),
        in_specs=[smem] * 2 + [anywhere] * 3 + [vmem] * 5,
        out_specs=[vmem] * (2 + len(starts)),
        out_shape=[
            jax.ShapeDtypeStruct(parent.shape, jnp.float32),
            jax.ShapeDtypeStruct((levels, LANE), jnp.float32),
        ]
        + [edge] * len(starts),
        scratch_shapes=[
            pltpu.VMEM((span, pad_cols), jnp.float32),
            pltpu.VMEM((span, (NS + 1) * pad_cols), jnp.float32),
            pltpu.SMEM((3, levels), jnp.float32),
            pltpu.SemaphoreType.DMA((3,)),
        ]
        + [pltpu.VMEM((span, LANE), jnp.float32)] * wide,
        compiler_params=pltpu.CompilerParams(vmem_limit_bytes=VMEM_LIMIT),
        name="zonal",
    )(offset, band, relax, coef, merid_coef, got, low, high, parent, matrix)


def merid_kernel(
    band_ref, coef_ref, field_ref, before_ref, after_ref, out_ref, done_ref, done_sem, *halo_refs,
    par_rows, par_cols, bands, groups
):
    wide = len(halo_refs) // 2
    levels = field_ref.shape[0]
    size = levels // groups
    band = band_ref[0]
    keep_before = jnp.where(band > 0, 1.0, 0.0)
    keep_after = jnp.where(band < bands - 1, 1.0, 0.0)
    for k in range(wide):
        for i in range(NS):
            cols = slice(k * LANE, (k + 1) * LANE)
            halo_refs[k][pl.ds(SUB - NS + i, levels, stride=SUB), :] = before_ref[i, :, cols]
            halo_refs[wide + k][pl.ds(i, levels, stride=SUB), :] = after_ref[i, :, cols]
    row = lax.broadcasted_iota(jnp.int32, (SUB, wide * LANE), 0)

    def store(group):
        part = pl.ds(group * size, size)
        return pltpu.make_async_copy(done_ref.at[part], out_ref.at[part], done_sem.at[group])

    def one(level):
        at = pl.ds(pl.multiple_of(level * SUB, SUB), SUB)
        before = jnp.concatenate([r[at, :] for r in halo_refs[:wide]], axis=1)
        after = jnp.concatenate([r[at, :] for r in halo_refs[wide:]], axis=1)
        mine = field_ref[level]
        if wide * LANE > par_cols:
            mine = jnp.concatenate(
                [mine, jnp.zeros((par_rows, wide * LANE - par_cols), jnp.float32)], axis=1
            )
        tiles = [jnp.where((row >= SUB - NS) & (band > 0), before, 0.0)]
        tiles += [mine[j * SUB : (j + 1) * SUB] for j in range(par_rows // SUB)]
        tiles += [jnp.where((row < NS) & (band < bands - 1), after, 0.0)]
        coef = jnp.concatenate([coef_ref[pl.ds(level, 1), :]] * wide, axis=1)
        for sweep in range(NS):
            down = [pltpu.roll(t, 1, 0) for t in tiles]
            up = [pltpu.roll(t, SUB - 1, 0) for t in tiles]
            fresh = []
            for j, t in enumerate(tiles):
                prev = jnp.where(row == 0, down[j - 1], down[j]) if j else down[j]
                succ = jnp.where(row == SUB - 1, up[j + 1], up[j]) if j + 1 < len(tiles) else up[j]
                fresh.append(t + coef * (prev + succ - 2.0 * t))
            tiles = fresh
            if sweep + 1 < NS:
                tiles[0] = tiles[0] * keep_before
                tiles[-1] = tiles[-1] * keep_after
        done_ref[level] = jnp.concatenate(tiles[1:-1], axis=0)[:, :par_cols]

    def body(group, carry):
        for k in range(size):
            one(group * size + k)
        store(group).start()
        return carry

    lax.fori_loop(0, groups, body, 0)
    for group in range(groups):
        store(group).wait()


def merid(band, coef, field, before, after, bands):
    levels, par_rows, par_cols = field.shape
    wide = lane_blocks(par_cols)
    groups = 4
    smem = pl.BlockSpec(memory_space=pltpu.SMEM)
    vmem = pl.BlockSpec(memory_space=pltpu.VMEM)
    return pl.pallas_call(
        functools.partial(
            merid_kernel, par_rows=par_rows, par_cols=par_cols, bands=bands, groups=groups
        ),
        in_specs=[smem] + [vmem] * 4,
        out_specs=pl.BlockSpec(memory_space=pl.ANY),
        out_shape=jax.ShapeDtypeStruct(field.shape, jnp.float32),
        scratch_shapes=[
            pltpu.VMEM(field.shape, jnp.float32),
            pltpu.SemaphoreType.DMA((groups,)),
        ]
        + [pltpu.VMEM((levels * SUB, LANE), jnp.float32)] * (2 * wide),
        compiler_params=pltpu.CompilerParams(vmem_limit_bytes=VMEM_LIMIT),
        name="merid",
    )(band, coef, field, before, after)


def turn(value, steps):
    count = lax.axis_size("lon")
    return lax.ppermute(value, "lon", [(i, (i + steps) % count) for i in range(count)])


def on_device(nest_field, nest_area, parent_field, nest_offset, relax_rate, zonal_coef, merid_coef):
    levels, par_rows, par_cols = parent_field.shape
    frame = par_cols + 2 * HALO
    cycle = lax.axis_size("lon")
    bands = lax.axis_size("band")
    span = levels * par_rows

    places = lax.div(nest_offset[0], 3)
    steps = lax.rem(lax.div(places, par_cols), cycle)
    slot = lax.div(lax.rem(places, par_cols) + HALO, QUANTUM)
    band = lax.axis_index("band").astype(jnp.int32)[None]
    bins = -(-frame // QUANTUM)

    near, far, spill, matrix = restrict(
        nest_field, nest_area, nest_offset, parent_field
    )
    low = turn(spill[5 * SUB :], 1)
    high = turn(spill[4 * SUB : 5 * SUB], -1)

    def branch(step, number):
        start = number * QUANTUM
        count = min(start + QUANTUM, frame)

        def send(near, far, spill):
            got_near = turn(near[start:], step)
            got_far = turn(far[: SUB + count], step + 1)
            if number == 0:
                cut = par_cols + 2 * HALO - SUB
                got_near = jnp.concatenate(
                    [got_near[:cut], got_near[cut:] + turn(spill[: 2 * SUB], step - 1)], axis=0
                )
            if number == bins - 1:
                cut = 2 * SUB
                got_far = jnp.concatenate(
                    [got_far[:cut] + turn(spill[2 * SUB : 4 * SUB], step + 2), got_far[cut:]], axis=0
                )
            gap = start + QUANTUM - count
            pieces = [got_far] + ([jnp.zeros((gap, span), jnp.float32)] if gap else []) + [got_near]
            return jnp.concatenate(pieces, axis=0)

        return send

    branches = [branch(step, number) for step in range(cycle) for number in range(bins)]
    got = lax.switch(steps * bins + slot, branches, near, far, spill)

    if bands == 2:
        starts = ((par_rows - NS, -(par_rows - NS)),)
    else:
        starts = ((par_rows - NS, 0), (0, 0))
    field, coef, *edges = zonal(
        nest_offset, band, relax_rate, zonal_coef, merid_coef, got, low, high, parent_field,
        matrix, starts,
    )
    if bands == 2:
        other = lax.ppermute(edges[0], "band", [(0, 1), (1, 0)])
        north, south = other, other
    else:
        north = lax.ppermute(edges[0], "band", [(i, i + 1) for i in range(bands - 1)])
        south = lax.ppermute(edges[1], "band", [(i + 1, i) for i in range(bands - 1)])
    return merid(band, coef, field, north, south, bands)


def solution(mesh):
    placed = (P(None, "band", "lon"), P("band", "lon"), P(None, "band", "lon"), P(), P(), P(), P())
    return jax.shard_map(
        on_device, mesh=mesh, in_specs=placed, out_specs=P(None, "band", "lon"), check_vma=False
    )
```

```python
import functools
import math

import jax
import jax.numpy as jnp
from jax import lax
from jax.experimental import pallas as pl
from jax.experimental.pallas import tpu as pltpu
from jax.sharding import PartitionSpec as P

NS = 3
BINOMIAL = [math.comb(NS, p) for p in range(NS + 1)]
HALO = 4
LANE = 128
VMEM_LIMIT = 16 << 20
EARLY_FLOPS = 6_000_000_000
QUANTUM = 40
SUB = 8


def lane_blocks(width):
    return -(-width // LANE)


def split_dot(value, selector, parts):
    total = None
    for part in range(parts):
        piece = value.astype(jnp.bfloat16)
        term = jnp.dot(piece, selector, preferred_element_type=jnp.float32)
        total = term if total is None else total + term
        if part + 1 < parts:
            value = value - piece.astype(jnp.float32)
    return total


def zonal_matrix(frame, par_cols, pad_cols, power):
    lane = lax.broadcasted_iota(jnp.int32, (pad_cols, pad_cols), 0)
    target = lax.broadcasted_iota(jnp.int32, (pad_cols, pad_cols), 1)
    low = frame + SUB - HALO
    column = jnp.where(
        lane < frame,
        lane,
        jnp.where(
            (lane >= low) & (lane < frame + SUB),
            lane - low,
            jnp.where(
                (lane >= frame + SUB) & (lane < frame + SUB + HALO),
                lane - SUB - HALO,
                -pad_cols,
            ),
        ),
    )
    apart = jnp.abs(column - HALO - target)
    weights = [1]
    for _ in range(power):
        weights = [
            x - 2 * y + z
            for x, y, z in zip([0, 0] + weights, [0] + weights + [0], weights + [0, 0])
        ]
    out = jnp.zeros((pad_cols, pad_cols), jnp.float32)
    for distance in range(power + 1):
        out = jnp.where(apart == distance, float(weights[power + distance]), out)
    return jnp.where(target < par_cols, out, 0.0).astype(jnp.bfloat16)


def prepare_kernel(offset_ref, sel_ref, mat_ref, *, frame, par_cols, pad_cols, nest_width):
    offset = offset_ref[0]
    g = lax.broadcasted_iota(jnp.int32, sel_ref.shape, 0)
    c = lax.broadcasted_iota(jnp.int32, sel_ref.shape, 1)
    low = 3 * (c - (offset // 3 % par_cols + HALO) % SUB) - offset % 3
    hit = (g >= low) & (g < low + 3) & (g < nest_width)
    sel_ref[...] = jnp.where(hit, 1.0, 0.0).astype(jnp.bfloat16)
    for power in range(NS + 1):
        mat_ref[:, power * pad_cols : (power + 1) * pad_cols] = zonal_matrix(
            frame, par_cols, pad_cols, power
        )


def prepare(nest_offset, nest_width, par_cols):
    frame = par_cols + 2 * HALO
    pad_cols = padded_width(frame)
    vmem = pl.BlockSpec(memory_space=pltpu.VMEM)
    return pl.pallas_call(
        functools.partial(
            prepare_kernel,
            frame=frame,
            par_cols=par_cols,
            pad_cols=pad_cols,
            nest_width=nest_width,
        ),
        in_specs=[pl.BlockSpec(memory_space=pltpu.SMEM)],
        out_specs=[vmem] * 2,
        out_shape=[
            jax.ShapeDtypeStruct((lane_blocks(nest_width) * LANE, pad_cols), jnp.bfloat16),
            jax.ShapeDtypeStruct((pad_cols, (NS + 1) * pad_cols), jnp.bfloat16),
        ],
        compiler_params=pltpu.CompilerParams(vmem_limit_bytes=VMEM_LIMIT),
        cost_estimate=pl.CostEstimate(
            flops=EARLY_FLOPS, bytes_accessed=4 * LANE * LANE, transcendentals=0
        ),
        name="prepare",
    )(nest_offset)


def edges_kernel(parent_ref, after_ref, last_ref, first_ref, *, par_cols):
    del after_ref
    span = first_ref.shape[1]
    low = (par_cols - SUB) // LANE * LANE
    wide = min(LANE, par_cols)
    left = parent_ref[:, :, :wide].reshape(span, wide)
    right = parent_ref[:, :, low:].reshape(span, par_cols - low)
    first_ref[...] = left.T[:SUB]
    last_ref[...] = right.T[par_cols - low - SUB :]


def parent_edges(parent, after):
    levels, par_rows, par_cols = parent.shape
    vmem = pl.BlockSpec(memory_space=pltpu.VMEM)
    return pl.pallas_call(
        functools.partial(edges_kernel, par_cols=par_cols),
        in_specs=[vmem, pl.BlockSpec(memory_space=pl.ANY)],
        out_specs=[vmem] * 2,
        out_shape=[jax.ShapeDtypeStruct((SUB, levels * par_rows), jnp.float32)] * 2,
        compiler_params=pltpu.CompilerParams(vmem_limit_bytes=VMEM_LIMIT),
        name="edges",
    )(parent, after)


def restrict_kernel(
    offset_ref, area_ref, nest_ref, sel_ref, relax_ref, zonal_ref, merid_ref,
    near_ref, far_ref, spill_ref, coef_ref,
    stage_ref, prod_ref, table_ref, table_sem,
    *, blocks, nest_width, par_cols, par_rows, frame, chunks, pad_cols
):
    level_block = LANE // par_rows
    nest_rows = 3 * par_rows
    fetches = [
        pltpu.make_async_copy(source, table_ref.at[k], table_sem.at[k])
        for k, source in enumerate((relax_ref, zonal_ref, merid_ref))
    ]
    for fetch in fetches:
        fetch.start()
    offset = offset_ref[0]
    place = offset // 3 % par_cols + HALO
    tile = place // SUB
    stage_ref[...] = jnp.zeros_like(stage_ref)

    def columns(value, b):
        width = min(LANE, nest_width - b * LANE)
        piece = value[..., b * LANE : b * LANE + width]
        if width == LANE:
            return piece
        return jnp.concatenate(
            [piece, jnp.zeros(piece.shape[:-1] + (LANE - width,), jnp.float32)], axis=-1
        )

    def row_sums(b, count):
        total = None
        for i in range(3):
            term = prod_ref[b, pl.ds(i, count, stride=3), :]
            total = term if total is None else total + term
        return total

    for b in range(blocks):
        prod_ref[b, :nest_rows, :] = columns(area_ref[...], b)
    total = jnp.concatenate([row_sums(b, par_rows) for b in range(blocks)], axis=1)
    compact = split_dot(total, sel_ref[...], 3)
    wide = jnp.concatenate([compact, jnp.zeros_like(compact)], axis=1)
    lanes = lax.broadcasted_iota(jnp.int32, (par_rows, pad_cols), 1)

    def packed(shift):
        moved = pltpu.roll(wide, (tile * SUB + shift + 2 * pad_cols) % (2 * pad_cols), 1)
        return jnp.where(lanes < frame, moved[:, :pad_cols], 0.0)

    def put(ref, row, part):
        ref[row : row + SUB, :] = jnp.zeros((SUB, ref.shape[1]), jnp.float32)
        for k in range(par_rows // SUB):
            ref[row : row + SUB, k * pad_cols : (k + 1) * pad_cols] = part[
                k * SUB : (k + 1) * SUB
            ]

    put(near_ref, frame, packed(0))
    put(far_ref, 0, packed(-par_cols))
    edge = lanes >= par_cols
    put(spill_ref, SUB, jnp.where(edge & (tile == 0), packed(par_cols), 0.0))
    last = tile == par_cols // SUB
    put(spill_ref, 2 * SUB, jnp.where((lanes < SUB) & last, packed(-2 * par_cols), 0.0))

    for chunk in range(chunks):
        for b in range(blocks):
            area = columns(area_ref[...], b)
            for k in range(level_block):
                prod_ref[b, k * nest_rows : (k + 1) * nest_rows, :] = area * columns(
                    nest_ref[chunk * level_block + k], b
                )
        sums = jnp.concatenate([row_sums(b, LANE) for b in range(blocks)], axis=1)
        turned = split_dot(sums, sel_ref[...], 2).T
        stage_ref[pl.ds(pl.multiple_of(tile * SUB, SUB), frame), :] = turned[:frame]
        cols = slice(chunk * LANE, (chunk + 1) * LANE)
        near_ref[:frame, cols] = stage_ref[:frame, :]
        far_ref[SUB:, cols] = stage_ref[par_cols : par_cols + frame, :]
        spill_ref[:SUB, cols] = stage_ref[:SUB, :]
        spill_ref[3 * SUB :, cols] = stage_ref[2 * par_cols : 2 * par_cols + SUB, :]

    for fetch in fetches:
        fetch.wait()
    levels = table_ref.shape[1]
    for k in range(table_ref.shape[0]):
        for level in range(levels):
            coef_ref[k * levels + level : k * levels + level + 1, :] = jnp.full(
                (1, LANE), table_ref[k, level], jnp.float32
            )


def padded_width(frame):
    return lane_blocks(frame + 2 * SUB) * LANE


def restrict(nest_field, nest_area, nest_offset, selector, coefs, par_cols):
    levels, nest_rows, nest_width = nest_field.shape
    par_rows = nest_rows // 3
    frame = par_cols + 2 * HALO
    pad_cols = padded_width(frame)
    blocks = lane_blocks(nest_width)
    level_block = LANE // par_rows
    span = levels * par_rows
    chunks = levels // level_block
    smem = pl.BlockSpec(memory_space=pltpu.SMEM)
    vmem = pl.BlockSpec(memory_space=pltpu.VMEM)
    sizes = (frame + SUB, frame + SUB, 4 * SUB)
    return pl.pallas_call(
        functools.partial(
            restrict_kernel,
            blocks=blocks,
            nest_width=nest_width,
            par_cols=par_cols,
            par_rows=par_rows,
            frame=frame,
            chunks=chunks,
            pad_cols=pad_cols,
        ),
        in_specs=[smem, vmem, vmem, vmem] + [pl.BlockSpec(memory_space=pl.ANY)] * len(coefs),
        out_specs=[vmem] * (len(sizes) + 1),
        out_shape=[jax.ShapeDtypeStruct((n, span), jnp.float32) for n in sizes]
        + [jax.ShapeDtypeStruct((len(coefs) * levels, LANE), jnp.float32)],
        scratch_shapes=[
            pltpu.VMEM((2 * par_cols + SUB, LANE), jnp.float32),
            pltpu.VMEM((blocks, level_block * nest_rows, LANE), jnp.float32),
            pltpu.SMEM((len(coefs), levels), jnp.float32),
            pltpu.SemaphoreType.DMA((len(coefs),)),
        ],
        compiler_params=pltpu.CompilerParams(vmem_limit_bytes=VMEM_LIMIT),
        name="restrict",
    )(nest_offset, nest_area, nest_field, selector, *coefs)


def bin_start(offset, par_cols):
    place = lax.rem(lax.div(offset, 3), par_cols) + HALO
    return lax.div(place, QUANTUM) * QUANTUM


def edge_rows(levels, par_cols):
    halves = par_cols % LANE == LANE // 2 and levels % (2 * SUB) == 0
    whole = par_cols // LANE if halves else lane_blocks(par_cols)
    return NS * levels * whole, NS * levels // 2 if halves else 0


def place_edge(edge_ref, i, w, picked, par_cols):
    levels = picked.shape[0]
    whole, shared = edge_rows(levels, par_cols)
    at = (w * NS + i) * levels
    if at < whole:
        edge_ref[at : at + levels, :] = picked
        return
    half = levels // 2
    lane = lax.broadcasted_iota(jnp.int32, (half, LANE), 1)
    joined = jnp.where(
        lane < LANE // 2, picked[:half], pltpu.roll(picked[half:], LANE // 2, 1)
    )
    edge_ref[whole + i * half : whole + (i + 1) * half, :] = joined


def take_edge(edge_ref, i, w, levels, par_cols):
    whole, shared = edge_rows(levels, par_cols)
    at = (w * NS + i) * levels
    if at < whole:
        return edge_ref[at : at + levels, :]
    half = levels // 2
    joined = edge_ref[whole + i * half : whole + (i + 1) * half, :]
    return jnp.concatenate([joined, pltpu.roll(joined, LANE // 2, 1)], axis=0)


def zonal_kernel(
    offset_ref, band_ref, coef_ref, got_ref, low_ref, high_ref, parent_ref,
    mat_ref, out_ref, *rest, frame, par_cols, par_rows, pad_cols, starts
):
    edge_refs = rest[: len(starts)]
    num_ref, pow_ref, *z_refs = rest[len(starts) :]
    levels = parent_ref.shape[0]

    def coefficient(kind, level, width):
        row = coef_ref[kind * levels + level : kind * levels + level + 1, :]
        return jnp.concatenate([row] * lane_blocks(width), axis=1)[:, :width]

    start = bin_start(offset_ref[0], par_cols)
    level_block = LANE // par_rows
    chunks = levels // level_block
    count = got_ref.shape[0]
    packed = got_ref[:SUB, :] + got_ref[count - SUB :, :]
    area = jnp.concatenate(
        [packed[:, k * pad_cols : (k + 1) * pad_cols] for k in range(par_rows // SUB)], axis=0
    )
    inverse = 1.0 / area
    inside = lax.broadcasted_iota(jnp.int32, (par_rows, pad_cols), 1) < frame
    rows = lax.broadcasted_iota(jnp.int32, (frame, LANE), 0)
    for chunk in range(chunks):
        cols = slice(chunk * LANE, (chunk + 1) * LANE)
        num = jnp.where(rows < start + QUANTUM, got_ref[SUB : SUB + frame, cols], 0.0) + jnp.where(
            rows >= start, got_ref[SUB + QUANTUM : SUB + QUANTUM + frame, cols], 0.0
        )
        rest_rows = pad_cols - frame - 2 * SUB
        num_ref[cols, :] = jnp.concatenate(
            [num, low_ref[:, cols], high_ref[:, cols], jnp.zeros((rest_rows, LANE), jnp.float32)],
            axis=0,
        ).T
    for chunk in range(chunks):
        fields = []
        for k in range(level_block):
            level = chunk * level_block + k
            relax = coefficient(0, level, pad_cols)
            own = parent_ref[level]
            own = jnp.concatenate(
                [own, jnp.zeros((par_rows, pad_cols - par_cols), jnp.float32)], axis=1
            )
            own = pltpu.roll(own, HALO, 1)
            scale = jnp.where(inside, relax * inverse, 1.0 - relax)
            at = slice(level * par_rows, (level + 1) * par_rows)
            fields.append(num_ref[at, :] * scale + (1.0 - relax) * own)
        field = jnp.concatenate(fields, axis=0)
        high = field.astype(jnp.bfloat16)
        low = (field - high.astype(jnp.float32)).astype(jnp.bfloat16)
        pow_ref[chunk * LANE : (chunk + 1) * LANE, :] = jnp.dot(
            high, mat_ref[...], preferred_element_type=jnp.float32
        ) + jnp.dot(low, mat_ref[...], preferred_element_type=jnp.float32)
    for level in range(levels):
        coef = coefficient(1, level, par_cols)
        at = slice(level * par_rows, (level + 1) * par_rows)
        term = [pow_ref[at, p * pad_cols : p * pad_cols + par_cols] for p in range(NS + 1)]
        field = term[0]
        scale = coef
        for p in range(1, NS + 1):
            field = field + (scale * float(BINOMIAL[p])) * term[p]
            scale = scale * coef
        out_ref[level] = field
        for w, z_ref in enumerate(z_refs):
            width = min(LANE, par_cols - w * LANE)
            z_ref[at, :width] = field[:, w * LANE : w * LANE + width]
    for edge_ref, (fixed, by_band) in zip(edge_refs, starts):
        for i in range(NS):
            base = fixed + i + (by_band * band_ref[0] if by_band else 0)
            for w, z_ref in enumerate(z_refs):
                picked = z_ref[pl.ds(base, levels, stride=par_rows), :]
                place_edge(edge_ref, i, w, picked, par_cols)


def zonal(offset, band, table, got, low, high, parent, matrix, starts):
    levels, par_rows, par_cols = parent.shape
    frame = par_cols + 2 * HALO
    pad_cols = padded_width(frame)
    wide = lane_blocks(par_cols)
    span = levels * par_rows
    smem = pl.BlockSpec(memory_space=pltpu.SMEM)
    vmem = pl.BlockSpec(memory_space=pltpu.VMEM)
    edge = jax.ShapeDtypeStruct((sum(edge_rows(levels, par_cols)), LANE), jnp.float32)
    return pl.pallas_call(
        functools.partial(
            zonal_kernel,
            frame=frame,
            par_cols=par_cols,
            par_rows=par_rows,
            pad_cols=pad_cols,
            starts=starts,
        ),
        in_specs=[smem] * 2 + [vmem] * 6,
        out_specs=[vmem] * (1 + len(starts)),
        out_shape=[
            jax.ShapeDtypeStruct(parent.shape, jnp.float32),
        ]
        + [edge] * len(starts),
        scratch_shapes=[
            pltpu.VMEM((span, pad_cols), jnp.float32),
            pltpu.VMEM((span, (NS + 1) * pad_cols), jnp.float32),
        ]
        + [pltpu.VMEM((span, LANE), jnp.float32)] * wide,
        compiler_params=pltpu.CompilerParams(vmem_limit_bytes=VMEM_LIMIT),
        name="zonal",
    )(offset, band, table, got, low, high, parent, matrix)


def merid_kernel(
    band_ref, coef_ref, field_ref, before_ref, after_ref, out_ref, done_ref, done_sem, *halo_refs,
    par_rows, par_cols, bands, groups
):
    wide = len(halo_refs) // 2
    levels = field_ref.shape[0]
    size = levels // groups
    band = band_ref[0]
    keep_before = jnp.where(band > 0, 1.0, 0.0)
    keep_after = jnp.where(band < bands - 1, 1.0, 0.0)
    for k in range(wide):
        for i in range(NS):
            halo_refs[k][pl.ds(SUB - NS + i, levels, stride=SUB), :] = take_edge(
                before_ref, i, k, levels, par_cols
            )
            halo_refs[wide + k][pl.ds(i, levels, stride=SUB), :] = take_edge(
                after_ref, i, k, levels, par_cols
            )
    row = lax.broadcasted_iota(jnp.int32, (SUB, wide * LANE), 0)

    def store(group):
        part = pl.ds(group * size, size)
        return pltpu.make_async_copy(done_ref.at[part], out_ref.at[part], done_sem.at[group])

    def one(level):
        at = pl.ds(pl.multiple_of(level * SUB, SUB), SUB)
        before = jnp.concatenate([r[at, :] for r in halo_refs[:wide]], axis=1)
        after = jnp.concatenate([r[at, :] for r in halo_refs[wide:]], axis=1)
        mine = field_ref[level]
        if wide * LANE > par_cols:
            mine = jnp.concatenate(
                [mine, jnp.zeros((par_rows, wide * LANE - par_cols), jnp.float32)], axis=1
            )
        tiles = [jnp.where((row >= SUB - NS) & (band > 0), before, 0.0)]
        tiles += [mine[j * SUB : (j + 1) * SUB] for j in range(par_rows // SUB)]
        tiles += [jnp.where((row < NS) & (band < bands - 1), after, 0.0)]
        coef = jnp.concatenate([coef_ref[pl.ds(2 * levels + level, 1), :]] * wide, axis=1)
        keep = 1.0 - 2.0 * coef
        for sweep in range(NS):
            down = [pltpu.roll(t, 1, 0) for t in tiles]
            up = [pltpu.roll(t, SUB - 1, 0) for t in tiles]
            fresh = []
            for j, t in enumerate(tiles):
                prev = jnp.where(row == 0, down[j - 1], down[j]) if j else down[j]
                succ = jnp.where(row == SUB - 1, up[j + 1], up[j]) if j + 1 < len(tiles) else up[j]
                fresh.append(keep * t + coef * (prev + succ))
            tiles = fresh
            if sweep + 1 < NS:
                tiles[0] = tiles[0] * keep_before
                tiles[-1] = tiles[-1] * keep_after
        done_ref[level] = jnp.concatenate(tiles[1:-1], axis=0)[:, :par_cols]

    def body(group, carry):
        for k in range(size):
            one(group * size + k)
        store(group).start()
        return carry

    lax.fori_loop(0, groups, body, 0)
    for group in range(groups):
        store(group).wait()


def merid(band, coef, field, before, after, bands):
    levels, par_rows, par_cols = field.shape
    wide = lane_blocks(par_cols)
    groups = 4
    smem = pl.BlockSpec(memory_space=pltpu.SMEM)
    vmem = pl.BlockSpec(memory_space=pltpu.VMEM)
    return pl.pallas_call(
        functools.partial(
            merid_kernel, par_rows=par_rows, par_cols=par_cols, bands=bands, groups=groups
        ),
        in_specs=[smem] + [vmem] * 4,
        out_specs=pl.BlockSpec(memory_space=pl.ANY),
        out_shape=jax.ShapeDtypeStruct(field.shape, jnp.float32),
        scratch_shapes=[
            pltpu.VMEM(field.shape, jnp.float32),
            pltpu.SemaphoreType.DMA((groups,)),
        ]
        + [pltpu.VMEM((levels * SUB, LANE), jnp.float32)] * (2 * wide),
        compiler_params=pltpu.CompilerParams(vmem_limit_bytes=VMEM_LIMIT),
        name="merid",
    )(band, coef, field, before, after)


def turn(value, steps):
    count = lax.axis_size("lon")
    return lax.ppermute(value, "lon", [(i, (i + steps) % count) for i in range(count)])


def on_device(nest_field, nest_area, parent_field, nest_offset, relax_rate, zonal_coef, merid_coef):
    levels, par_rows, par_cols = parent_field.shape
    frame = par_cols + 2 * HALO
    cycle = lax.axis_size("lon")
    bands = lax.axis_size("band")
    span = levels * par_rows

    places = lax.div(nest_offset[0], 3)
    steps = lax.rem(lax.div(places, par_cols), cycle)
    slot = lax.div(lax.rem(places, par_cols) + HALO, QUANTUM)
    band = lax.axis_index("band").astype(jnp.int32)[None]
    bins = -(-frame // QUANTUM)

    selector, matrix = prepare(nest_offset, nest_field.shape[2], par_cols)
    last, first = parent_edges(parent_field, selector)
    low = turn(last, 1)
    high = turn(first, -1)
    coefs = (relax_rate, zonal_coef, merid_coef)
    near, far, spill, table = restrict(
        nest_field, nest_area, nest_offset, selector, coefs, par_cols
    )

    def branch(step, number):
        start = number * QUANTUM
        count = min(start + QUANTUM, frame)

        def send(near, far, spill):
            got_near = turn(near[start:], step)
            got_far = turn(far[: SUB + count], step + 1)
            if number == 0:
                cut = par_cols + 2 * HALO - SUB
                got_near = jnp.concatenate(
                    [got_near[:cut], got_near[cut:] + turn(spill[: 2 * SUB], step - 1)], axis=0
                )
            if number == bins - 1:
                cut = 2 * SUB
                got_far = jnp.concatenate(
                    [got_far[:cut] + turn(spill[2 * SUB :], step + 2), got_far[cut:]], axis=0
                )
            gap = start + QUANTUM - count
            pieces = [got_far] + ([jnp.zeros((gap, span), jnp.float32)] if gap else []) + [got_near]
            return jnp.concatenate(pieces, axis=0)

        return send

    branches = [branch(step, number) for step in range(1, cycle) for number in range(bins)]
    got = lax.switch((steps - 1) * bins + slot, branches, near, far, spill)

    if bands == 2:
        starts = ((par_rows - NS, -(par_rows - NS)),)
    else:
        starts = ((par_rows - NS, 0), (0, 0))
    field, *edges = zonal(
        nest_offset, band, table, got, low, high, parent_field, matrix, starts
    )
    if bands == 2:
        other = lax.ppermute(edges[0], "band", [(0, 1), (1, 0)])
        north, south = other, other
    else:
        north = lax.ppermute(edges[0], "band", [(i, i + 1) for i in range(bands - 1)])
        south = lax.ppermute(edges[1], "band", [(i + 1, i) for i in range(bands - 1)])
    return merid(band, table, field, north, south, bands)


def solution(mesh):
    placed = (P(None, "band", "lon"), P("band", "lon"), P(None, "band", "lon"), P(), P(), P(), P())
    return jax.shard_map(
        on_device, mesh=mesh, in_specs=placed, out_specs=P(None, "band", "lon"), check_vma=False
    )
```

```python
import functools
import math

import jax
import jax.numpy as jnp
from jax import lax
from jax.experimental import pallas as pl
from jax.experimental.pallas import tpu as pltpu
from jax.sharding import PartitionSpec as P

NS = 3
BINOMIAL = [math.comb(NS, p) for p in range(NS + 1)]
HALO = 4
LANE = 128
VMEM_LIMIT = 16 << 20
EARLY_FLOPS = 6_000_000_000
QUANTUM = 40
SUB = 8


def lane_blocks(width):
    return -(-width // LANE)


def split_dot(value, selector, parts):
    total = None
    for part in range(parts):
        piece = value.astype(jnp.bfloat16)
        term = jnp.dot(piece, selector, preferred_element_type=jnp.float32)
        total = term if total is None else total + term
        if part + 1 < parts:
            value = value - piece.astype(jnp.float32)
    return total


def zonal_matrix(frame, par_cols, pad_cols, power):
    lane = lax.broadcasted_iota(jnp.int32, (pad_cols, pad_cols), 0)
    target = lax.broadcasted_iota(jnp.int32, (pad_cols, pad_cols), 1)
    low = frame + SUB - HALO
    column = jnp.where(
        lane < frame,
        lane,
        jnp.where(
            (lane >= low) & (lane < frame + SUB),
            lane - low,
            jnp.where(
                (lane >= frame + SUB) & (lane < frame + SUB + HALO),
                lane - SUB - HALO,
                -pad_cols,
            ),
        ),
    )
    apart = jnp.abs(column - HALO - target)
    weights = [1]
    for _ in range(power):
        weights = [
            x - 2 * y + z
            for x, y, z in zip([0, 0] + weights, [0] + weights + [0], weights + [0, 0])
        ]
    out = jnp.zeros((pad_cols, pad_cols), jnp.float32)
    for distance in range(power + 1):
        out = jnp.where(apart == distance, float(weights[power + distance]), out)
    return jnp.where(target < par_cols, out, 0.0).astype(jnp.bfloat16)


def prepare_kernel(mat_ref, *, frame, par_cols, pad_cols):
    for power in range(NS + 1):
        mat_ref[:, power * pad_cols : (power + 1) * pad_cols] = zonal_matrix(
            frame, par_cols, pad_cols, power
        )


def prepare(par_cols):
    frame = par_cols + 2 * HALO
    pad_cols = padded_width(frame)
    return pl.pallas_call(
        functools.partial(prepare_kernel, frame=frame, par_cols=par_cols, pad_cols=pad_cols),
        out_specs=pl.BlockSpec(memory_space=pltpu.VMEM),
        out_shape=jax.ShapeDtypeStruct((pad_cols, (NS + 1) * pad_cols), jnp.bfloat16),
        compiler_params=pltpu.CompilerParams(vmem_limit_bytes=VMEM_LIMIT),
        cost_estimate=pl.CostEstimate(
            flops=EARLY_FLOPS, bytes_accessed=4 * LANE * LANE, transcendentals=0
        ),
        name="prepare",
    )()


def edges_kernel(offset_ref, parent_ref, after_ref, last_ref, first_ref, sel_ref, *, par_cols, nest_width):
    del after_ref
    offset = offset_ref[0]
    g = lax.broadcasted_iota(jnp.int32, sel_ref.shape, 0)
    c = lax.broadcasted_iota(jnp.int32, sel_ref.shape, 1)
    low = 3 * (c - (offset // 3 % par_cols + HALO) % SUB) - offset % 3
    hit = (g >= low) & (g < low + 3) & (g < nest_width)
    sel_ref[...] = jnp.where(hit, 1.0, 0.0).astype(jnp.bfloat16)
    span = first_ref.shape[1]
    low = (par_cols - SUB) // LANE * LANE
    wide = min(LANE, par_cols)
    left = parent_ref[:, :, :wide].reshape(span, wide)
    right = parent_ref[:, :, low:].reshape(span, par_cols - low)
    first_ref[...] = left.T[:SUB]
    last_ref[...] = right.T[par_cols - low - SUB :]


def parent_edges(nest_offset, parent, after, nest_width):
    levels, par_rows, par_cols = parent.shape
    vmem = pl.BlockSpec(memory_space=pltpu.VMEM)
    pad_cols = padded_width(par_cols + 2 * HALO)
    return pl.pallas_call(
        functools.partial(edges_kernel, par_cols=par_cols, nest_width=nest_width),
        in_specs=[
            pl.BlockSpec(memory_space=pltpu.SMEM), vmem, pl.BlockSpec(memory_space=pl.ANY)
        ],
        out_specs=[vmem] * 3,
        out_shape=[jax.ShapeDtypeStruct((SUB, levels * par_rows), jnp.float32)] * 2
        + [jax.ShapeDtypeStruct((lane_blocks(nest_width) * LANE, pad_cols), jnp.bfloat16)],
        compiler_params=pltpu.CompilerParams(vmem_limit_bytes=VMEM_LIMIT),
        name="edges",
    )(nest_offset, parent, after)


def restrict_kernel(
    offset_ref, area_ref, nest_ref, sel_ref, relax_ref, zonal_ref, merid_ref,
    near_ref, far_ref, spill_ref, coef_ref,
    stage_ref, prod_ref, table_ref, table_sem,
    *, blocks, nest_width, par_cols, par_rows, frame, chunks, pad_cols
):
    level_block = LANE // par_rows
    nest_rows = 3 * par_rows
    fetches = [
        pltpu.make_async_copy(source, table_ref.at[k], table_sem.at[k])
        for k, source in enumerate((relax_ref, zonal_ref, merid_ref))
    ]
    for fetch in fetches:
        fetch.start()
    offset = offset_ref[0]
    place = offset // 3 % par_cols + HALO
    tile = place // SUB
    stage_ref[...] = jnp.zeros_like(stage_ref)

    def columns(value, b):
        width = min(LANE, nest_width - b * LANE)
        piece = value[..., b * LANE : b * LANE + width]
        if width == LANE:
            return piece
        return jnp.concatenate(
            [piece, jnp.zeros(piece.shape[:-1] + (LANE - width,), jnp.float32)], axis=-1
        )

    def row_sums(b, count):
        total = None
        for i in range(3):
            term = prod_ref[b, pl.ds(i, count, stride=3), :]
            total = term if total is None else total + term
        return total

    for b in range(blocks):
        prod_ref[b, :nest_rows, :] = columns(area_ref[...], b)
    total = jnp.concatenate([row_sums(b, par_rows) for b in range(blocks)], axis=1)
    compact = split_dot(total, sel_ref[...], 3)
    wide = jnp.concatenate([compact, jnp.zeros_like(compact)], axis=1)
    lanes = lax.broadcasted_iota(jnp.int32, (par_rows, pad_cols), 1)

    def packed(shift):
        moved = pltpu.roll(wide, (tile * SUB + shift + 2 * pad_cols) % (2 * pad_cols), 1)
        return jnp.where(lanes < frame, moved[:, :pad_cols], 0.0)

    def put(ref, row, part):
        ref[row : row + SUB, :] = jnp.zeros((SUB, ref.shape[1]), jnp.float32)
        for k in range(par_rows // SUB):
            ref[row : row + SUB, k * pad_cols : (k + 1) * pad_cols] = part[
                k * SUB : (k + 1) * SUB
            ]

    put(near_ref, frame, packed(0))
    put(far_ref, 0, packed(-par_cols))
    edge = lanes >= par_cols
    put(spill_ref, SUB, jnp.where(edge & (tile == 0), packed(par_cols), 0.0))
    last = tile == par_cols // SUB
    put(spill_ref, 2 * SUB, jnp.where((lanes < SUB) & last, packed(-2 * par_cols), 0.0))

    for chunk in range(chunks):
        for b in range(blocks):
            area = columns(area_ref[...], b)
            for k in range(level_block):
                prod_ref[b, k * nest_rows : (k + 1) * nest_rows, :] = area * columns(
                    nest_ref[chunk * level_block + k], b
                )
        sums = jnp.concatenate([row_sums(b, LANE) for b in range(blocks)], axis=1)
        turned = split_dot(sums, sel_ref[...], 2).T
        stage_ref[pl.ds(pl.multiple_of(tile * SUB, SUB), frame), :] = turned[:frame]
        cols = slice(chunk * LANE, (chunk + 1) * LANE)
        near_ref[:frame, cols] = stage_ref[:frame, :]
        far_ref[SUB:, cols] = stage_ref[par_cols : par_cols + frame, :]
        spill_ref[:SUB, cols] = stage_ref[:SUB, :]
        spill_ref[3 * SUB :, cols] = stage_ref[2 * par_cols : 2 * par_cols + SUB, :]

    for fetch in fetches:
        fetch.wait()
    levels = table_ref.shape[1]
    for k in range(table_ref.shape[0]):
        for level in range(levels):
            coef_ref[k * levels + level : k * levels + level + 1, :] = jnp.full(
                (1, LANE), table_ref[k, level], jnp.float32
            )


def padded_width(frame):
    return lane_blocks(frame + 2 * SUB) * LANE


def restrict(nest_field, nest_area, nest_offset, selector, coefs, par_cols):
    levels, nest_rows, nest_width = nest_field.shape
    par_rows = nest_rows // 3
    frame = par_cols + 2 * HALO
    pad_cols = padded_width(frame)
    blocks = lane_blocks(nest_width)
    level_block = LANE // par_rows
    span = levels * par_rows
    chunks = levels // level_block
    smem = pl.BlockSpec(memory_space=pltpu.SMEM)
    vmem = pl.BlockSpec(memory_space=pltpu.VMEM)
    sizes = (frame + SUB, frame + SUB, 4 * SUB)
    return pl.pallas_call(
        functools.partial(
            restrict_kernel,
            blocks=blocks,
            nest_width=nest_width,
            par_cols=par_cols,
            par_rows=par_rows,
            frame=frame,
            chunks=chunks,
            pad_cols=pad_cols,
        ),
        in_specs=[smem, vmem, vmem, vmem] + [pl.BlockSpec(memory_space=pl.ANY)] * len(coefs),
        out_specs=[vmem] * (len(sizes) + 1),
        out_shape=[jax.ShapeDtypeStruct((n, span), jnp.float32) for n in sizes]
        + [jax.ShapeDtypeStruct((len(coefs) * levels, LANE), jnp.float32)],
        scratch_shapes=[
            pltpu.VMEM((2 * par_cols + SUB, LANE), jnp.float32),
            pltpu.VMEM((blocks, level_block * nest_rows, LANE), jnp.float32),
            pltpu.SMEM((len(coefs), levels), jnp.float32),
            pltpu.SemaphoreType.DMA((len(coefs),)),
        ],
        compiler_params=pltpu.CompilerParams(vmem_limit_bytes=VMEM_LIMIT),
        name="restrict",
    )(nest_offset, nest_area, nest_field, selector, *coefs)


def bin_start(offset, par_cols):
    place = lax.rem(lax.div(offset, 3), par_cols) + HALO
    return lax.div(place, QUANTUM) * QUANTUM


def edge_rows(levels, par_cols):
    halves = par_cols % LANE == LANE // 2 and levels % (2 * SUB) == 0
    whole = par_cols // LANE if halves else lane_blocks(par_cols)
    return NS * levels * whole, NS * levels // 2 if halves else 0


def place_edge(edge_ref, i, w, picked, par_cols):
    levels = picked.shape[0]
    whole, shared = edge_rows(levels, par_cols)
    at = (w * NS + i) * levels
    if at < whole:
        edge_ref[at : at + levels, :] = picked
        return
    half = levels // 2
    lane = lax.broadcasted_iota(jnp.int32, (half, LANE), 1)
    joined = jnp.where(
        lane < LANE // 2, picked[:half], pltpu.roll(picked[half:], LANE // 2, 1)
    )
    edge_ref[whole + i * half : whole + (i + 1) * half, :] = joined


def take_edge(edge_ref, i, w, levels, par_cols):
    whole, shared = edge_rows(levels, par_cols)
    at = (w * NS + i) * levels
    if at < whole:
        return edge_ref[at : at + levels, :]
    half = levels // 2
    joined = edge_ref[whole + i * half : whole + (i + 1) * half, :]
    return jnp.concatenate([joined, pltpu.roll(joined, LANE // 2, 1)], axis=0)


def zonal_kernel(
    offset_ref, band_ref, coef_ref, got_ref, low_ref, high_ref, parent_ref,
    mat_ref, out_ref, *rest, frame, par_cols, par_rows, pad_cols, starts
):
    edge_refs = rest[: len(starts)]
    num_ref, pow_ref, *z_refs = rest[len(starts) :]
    levels = parent_ref.shape[0]

    def coefficient(kind, level, width):
        row = coef_ref[kind * levels + level : kind * levels + level + 1, :]
        return jnp.concatenate([row] * lane_blocks(width), axis=1)[:, :width]

    start = bin_start(offset_ref[0], par_cols)
    level_block = LANE // par_rows
    chunks = levels // level_block
    count = got_ref.shape[0]
    packed = got_ref[:SUB, :] + got_ref[count - SUB :, :]
    area = jnp.concatenate(
        [packed[:, k * pad_cols : (k + 1) * pad_cols] for k in range(par_rows // SUB)], axis=0
    )
    inverse = 1.0 / area
    inside = lax.broadcasted_iota(jnp.int32, (par_rows, pad_cols), 1) < frame
    rows = lax.broadcasted_iota(jnp.int32, (frame, LANE), 0)
    for chunk in range(chunks):
        cols = slice(chunk * LANE, (chunk + 1) * LANE)
        num = jnp.where(rows < start + QUANTUM, got_ref[SUB : SUB + frame, cols], 0.0) + jnp.where(
            rows >= start, got_ref[SUB + QUANTUM : SUB + QUANTUM + frame, cols], 0.0
        )
        rest_rows = pad_cols - frame - 2 * SUB
        num_ref[cols, :] = jnp.concatenate(
            [num, low_ref[:, cols], high_ref[:, cols], jnp.zeros((rest_rows, LANE), jnp.float32)],
            axis=0,
        ).T
    for chunk in range(chunks):
        fields = []
        for k in range(level_block):
            level = chunk * level_block + k
            relax = coefficient(0, level, pad_cols)
            own = parent_ref[level]
            own = jnp.concatenate(
                [own, jnp.zeros((par_rows, pad_cols - par_cols), jnp.float32)], axis=1
            )
            own = pltpu.roll(own, HALO, 1)
            scale = jnp.where(inside, relax * inverse, 1.0 - relax)
            at = slice(level * par_rows, (level + 1) * par_rows)
            fields.append(num_ref[at, :] * scale + (1.0 - relax) * own)
        field = jnp.concatenate(fields, axis=0)
        high = field.astype(jnp.bfloat16)
        low = (field - high.astype(jnp.float32)).astype(jnp.bfloat16)
        pow_ref[chunk * LANE : (chunk + 1) * LANE, :] = jnp.dot(
            high, mat_ref[...], preferred_element_type=jnp.float32
        ) + jnp.dot(low, mat_ref[...], preferred_element_type=jnp.float32)
    for level in range(levels):
        coef = coefficient(1, level, par_cols)
        at = slice(level * par_rows, (level + 1) * par_rows)
        term = [pow_ref[at, p * pad_cols : p * pad_cols + par_cols] for p in range(NS + 1)]
        field = term[0]
        scale = coef
        for p in range(1, NS + 1):
            field = field + (scale * float(BINOMIAL[p])) * term[p]
            scale = scale * coef
        out_ref[level] = field
        for w, z_ref in enumerate(z_refs):
            width = min(LANE, par_cols - w * LANE)
            z_ref[at, :width] = field[:, w * LANE : w * LANE + width]
    for edge_ref, (fixed, by_band) in zip(edge_refs, starts):
        for i in range(NS):
            base = fixed + i + (by_band * band_ref[0] if by_band else 0)
            for w, z_ref in enumerate(z_refs):
                picked = z_ref[pl.ds(base, levels, stride=par_rows), :]
                place_edge(edge_ref, i, w, picked, par_cols)


def zonal(offset, band, table, got, low, high, parent, matrix, starts):
    levels, par_rows, par_cols = parent.shape
    frame = par_cols + 2 * HALO
    pad_cols = padded_width(frame)
    wide = lane_blocks(par_cols)
    span = levels * par_rows
    smem = pl.BlockSpec(memory_space=pltpu.SMEM)
    vmem = pl.BlockSpec(memory_space=pltpu.VMEM)
    edge = jax.ShapeDtypeStruct((sum(edge_rows(levels, par_cols)), LANE), jnp.float32)
    return pl.pallas_call(
        functools.partial(
            zonal_kernel,
            frame=frame,
            par_cols=par_cols,
            par_rows=par_rows,
            pad_cols=pad_cols,
            starts=starts,
        ),
        in_specs=[smem] * 2 + [vmem] * 6,
        out_specs=[vmem] * (1 + len(starts)),
        out_shape=[
            jax.ShapeDtypeStruct(parent.shape, jnp.float32),
        ]
        + [edge] * len(starts),
        scratch_shapes=[
            pltpu.VMEM((span, pad_cols), jnp.float32),
            pltpu.VMEM((span, (NS + 1) * pad_cols), jnp.float32),
        ]
        + [pltpu.VMEM((span, LANE), jnp.float32)] * wide,
        compiler_params=pltpu.CompilerParams(vmem_limit_bytes=VMEM_LIMIT),
        name="zonal",
    )(offset, band, table, got, low, high, parent, matrix)


def merid_kernel(
    band_ref, coef_ref, field_ref, before_ref, after_ref, out_ref, done_ref, done_sem, *halo_refs,
    par_rows, par_cols, bands, groups
):
    wide = len(halo_refs) // 2
    levels = field_ref.shape[0]
    size = levels // groups
    band = band_ref[0]
    keep_before = jnp.where(band > 0, 1.0, 0.0)
    keep_after = jnp.where(band < bands - 1, 1.0, 0.0)
    for k in range(wide):
        for i in range(NS):
            halo_refs[k][pl.ds(SUB - NS + i, levels, stride=SUB), :] = take_edge(
                before_ref, i, k, levels, par_cols
            )
            halo_refs[wide + k][pl.ds(i, levels, stride=SUB), :] = take_edge(
                after_ref, i, k, levels, par_cols
            )
    row = lax.broadcasted_iota(jnp.int32, (SUB, wide * LANE), 0)

    def store(group):
        part = pl.ds(group * size, size)
        return pltpu.make_async_copy(done_ref.at[part], out_ref.at[part], done_sem.at[group])

    def one(level):
        at = pl.ds(pl.multiple_of(level * SUB, SUB), SUB)
        before = jnp.concatenate([r[at, :] for r in halo_refs[:wide]], axis=1)
        after = jnp.concatenate([r[at, :] for r in halo_refs[wide:]], axis=1)
        mine = field_ref[level]
        if wide * LANE > par_cols:
            mine = jnp.concatenate(
                [mine, jnp.zeros((par_rows, wide * LANE - par_cols), jnp.float32)], axis=1
            )
        tiles = [jnp.where((row >= SUB - NS) & (band > 0), before, 0.0)]
        tiles += [mine[j * SUB : (j + 1) * SUB] for j in range(par_rows // SUB)]
        tiles += [jnp.where((row < NS) & (band < bands - 1), after, 0.0)]
        coef = jnp.concatenate([coef_ref[pl.ds(2 * levels + level, 1), :]] * wide, axis=1)
        keep = 1.0 - 2.0 * coef
        for sweep in range(NS):
            down = [pltpu.roll(t, 1, 0) for t in tiles]
            up = [pltpu.roll(t, SUB - 1, 0) for t in tiles]
            fresh = []
            for j, t in enumerate(tiles):
                prev = jnp.where(row == 0, down[j - 1], down[j]) if j else down[j]
                succ = jnp.where(row == SUB - 1, up[j + 1], up[j]) if j + 1 < len(tiles) else up[j]
                fresh.append(keep * t + coef * (prev + succ))
            tiles = fresh
            if sweep + 1 < NS:
                tiles[0] = tiles[0] * keep_before
                tiles[-1] = tiles[-1] * keep_after
        done_ref[level] = jnp.concatenate(tiles[1:-1], axis=0)[:, :par_cols]

    def body(group, carry):
        for k in range(size):
            one(group * size + k)
        store(group).start()
        return carry

    lax.fori_loop(0, groups, body, 0)
    for group in range(groups):
        store(group).wait()


def merid(band, coef, field, before, after, bands):
    levels, par_rows, par_cols = field.shape
    wide = lane_blocks(par_cols)
    groups = 4
    smem = pl.BlockSpec(memory_space=pltpu.SMEM)
    vmem = pl.BlockSpec(memory_space=pltpu.VMEM)
    return pl.pallas_call(
        functools.partial(
            merid_kernel, par_rows=par_rows, par_cols=par_cols, bands=bands, groups=groups
        ),
        in_specs=[smem] + [vmem] * 4,
        out_specs=pl.BlockSpec(memory_space=pl.ANY),
        out_shape=jax.ShapeDtypeStruct(field.shape, jnp.float32),
        scratch_shapes=[
            pltpu.VMEM(field.shape, jnp.float32),
            pltpu.SemaphoreType.DMA((groups,)),
        ]
        + [pltpu.VMEM((levels * SUB, LANE), jnp.float32)] * (2 * wide),
        compiler_params=pltpu.CompilerParams(vmem_limit_bytes=VMEM_LIMIT),
        name="merid",
    )(band, coef, field, before, after)


def turn(value, steps):
    count = lax.axis_size("lon")
    return lax.ppermute(value, "lon", [(i, (i + steps) % count) for i in range(count)])


def on_device(nest_field, nest_area, parent_field, nest_offset, relax_rate, zonal_coef, merid_coef):
    levels, par_rows, par_cols = parent_field.shape
    frame = par_cols + 2 * HALO
    cycle = lax.axis_size("lon")
    bands = lax.axis_size("band")
    span = levels * par_rows

    places = lax.div(nest_offset[0], 3)
    steps = lax.rem(lax.div(places, par_cols), cycle)
    slot = lax.div(lax.rem(places, par_cols) + HALO, QUANTUM)
    band = lax.axis_index("band").astype(jnp.int32)[None]
    bins = -(-frame // QUANTUM)

    matrix = prepare(par_cols)
    last, first, selector = parent_edges(
        nest_offset, parent_field, matrix, nest_field.shape[2]
    )
    low = turn(last, 1)
    high = turn(first, -1)
    coefs = (relax_rate, zonal_coef, merid_coef)
    near, far, spill, table = restrict(
        nest_field, nest_area, nest_offset, selector, coefs, par_cols
    )

    def branch(step, number):
        start = number * QUANTUM
        count = min(start + QUANTUM, frame)

        def send(near, far, spill):
            got_near = turn(near[start:], step)
            got_far = turn(far[: SUB + count], step + 1)
            if number == 0:
                cut = par_cols + 2 * HALO - SUB
                got_near = jnp.concatenate(
                    [got_near[:cut], got_near[cut:] + turn(spill[: 2 * SUB], step - 1)], axis=0
                )
            if number == bins - 1:
                cut = 2 * SUB
                got_far = jnp.concatenate(
                    [got_far[:cut] + turn(spill[2 * SUB :], step + 2), got_far[cut:]], axis=0
                )
            gap = start + QUANTUM - count
            pieces = [got_far] + ([jnp.zeros((gap, span), jnp.float32)] if gap else []) + [got_near]
            return jnp.concatenate(pieces, axis=0)

        return send

    branches = [branch(step, number) for step in range(1, cycle) for number in range(bins)]
    got = lax.switch((steps - 1) * bins + slot, branches, near, far, spill)

    if bands == 2:
        starts = ((par_rows - NS, -(par_rows - NS)),)
    else:
        starts = ((par_rows - NS, 0), (0, 0))
    field, *edges = zonal(
        nest_offset, band, table, got, low, high, parent_field, matrix, starts
    )
    if bands == 2:
        other = lax.ppermute(edges[0], "band", [(0, 1), (1, 0)])
        north, south = other, other
    else:
        north = lax.ppermute(edges[0], "band", [(i, i + 1) for i in range(bands - 1)])
        south = lax.ppermute(edges[1], "band", [(i + 1, i) for i in range(bands - 1)])
    return merid(band, table, field, north, south, bands)


def solution(mesh):
    placed = (P(None, "band", "lon"), P("band", "lon"), P(None, "band", "lon"), P(), P(), P(), P())
    return jax.shard_map(
        on_device, mesh=mesh, in_specs=placed, out_specs=P(None, "band", "lon"), check_vma=False
    )
```
